256 devices in a mesh: rows: 128 (over y_lo, x, z, core), feat: 2 (over y_hi).
Axes of the slice: x: 4, y: 4 (y_hi: 2, y_lo: 2; y = y_hi * 2 + y_lo), z: 8, core: 2. Of those that a mesh axis runs over, the one named last changes fastest.
Arguments:
- train_cells: bfloat16 [8192, 1536], P('rows', 'feat'), may hold values from -24 to 24
- test_cells: bfloat16 [4096, 1536], P('rows', 'feat'), may hold values from -24 to 24
- feat_weights: bfloat16 [4, 192, 192], replicated
- row_weights: bfloat16 [4, 192, 192], replicated
- mlp_up: bfloat16 [192, 768], replicated, may hold values from -0.4375 to 0.4375
- mlp_down: bfloat16 [768, 192], replicated, may hold values from -0.21875 to 0.21875
Outputs:
- train_out: bfloat16 [8192, 1536], P('rows', 'feat')
- test_out: bfloat16 [4096, 1536], P('rows', 'feat')
The draws below stay inside these ranges and needn't reach their ends.
All inputs are finite; a program needn't handle non-finite values.
Results may differ from the reference program's by a relative error of at most 0.017.
Values may be sent and summed in bfloat16 or wider, within the bound.
A program may use at most 128 MiB of HBM per device.

```python
import math
import jax
import jax.numpy as jnp
from jax import lax

E = 192
HEADS = 6
HD = 32
HID = 768
F = 8
TRAIN = 8192
TEST = 4096


def attention_weights(key, query_gain):
    split_keys = jax.random.split(key, 4)
    spread = E ** (-0.5)
    query_w = jax.random.normal(split_keys[0], (E, E), jnp.float32) * query_gain * spread
    key_w = jax.random.normal(split_keys[1], (E, E), jnp.float32) * spread
    value_w = jax.random.normal(split_keys[2], (E, E), jnp.float32) * spread
    output_w = jax.random.normal(split_keys[3], (E, E), jnp.float32) * spread
    return jnp.stack([query_w, key_w, value_w, output_w]).astype(jnp.bfloat16)


def draw_feat_weights(key, part):
    return attention_weights(jax.random.fold_in(key, 3), 1.5)


def draw_row_weights(key, part):
    return attention_weights(jax.random.fold_in(key, 5), 2.5)


def train_table(key):
    key_base = jax.random.fold_in(key, 0)
    table = jax.random.normal(key_base, (TRAIN, F, E), jnp.float32)
    return jnp.clip(table, -24.0, 24.0)


def draw_train_cells(key, part):
    return train_table(jax.random.fold_in(key, 11)).reshape(TRAIN, F * E).astype(jnp.bfloat16)


def draw_test_cells(key, part):
    fresh = jax.random.normal(jax.random.fold_in(key, 13), (TEST, F, E), jnp.float32)
    return jnp.clip(fresh, -24.0, 24.0).reshape(TEST, F * E).astype(jnp.bfloat16)


def bell_draw(key, dims, scale, limit, kind=jnp.bfloat16):
    values = scale * jax.random.normal(key, dims, jnp.float32)
    return jnp.clip(values, min=-limit, max=limit).astype(kind)


def setup_inputs(seed: int = 0) -> dict:
    key_list = jax.random.split(jax.random.key(seed), 7)
    train_cells = draw_train_cells(jax.random.fold_in(key_list[6], 71), 0)
    test_cells = draw_test_cells(jax.random.fold_in(key_list[6], 71), 0)
    feat_weights = draw_feat_weights(jax.random.fold_in(key_list[6], 71), 0)
    row_weights = draw_row_weights(jax.random.fold_in(key_list[6], 71), 0)
    mlp_up = bell_draw(key_list[4], (E, HID), E ** -0.5, 0.4375)
    mlp_down = bell_draw(key_list[5], (HID, E), HID ** -0.5, 0.21875)
    return dict(train_cells=train_cells, test_cells=test_cells, feat_weights=feat_weights, row_weights=row_weights, mlp_up=mlp_up, mlp_down=mlp_down)


eps_norm = 1e-05

def layer_norm(values_in):
    centred = values_in - lax.optimization_barrier(jnp.mean(values_in, axis=-1, keepdims=True))
    spread = lax.optimization_barrier(jnp.mean(centred * centred, axis=-1, keepdims=True))
    return centred * lax.rsqrt(spread + eps_norm)

def project(normed, weight):
    return jnp.dot(normed.reshape(-1, E), weight, preferred_element_type=jnp.float32)

def round_back(values_in):
    return lax.optimization_barrier(values_in.astype(jnp.bfloat16)).astype(jnp.float32)

def feature_attention(queries, key_heads, value_heads):
    scores = jnp.einsum('rqhd,rkhd->rhqk', queries.astype(jnp.float32), key_heads.astype(jnp.float32)) * HD ** (-0.5)
    row_peak = lax.optimization_barrier(jnp.max(scores, axis=-1, keepdims=True))
    weights = jnp.exp(scores - row_peak)
    totals = lax.optimization_barrier(jnp.sum(weights, axis=-1))
    mixture = jnp.einsum('rhqk,rkhd->rqhd', round_back(weights), value_heads.astype(jnp.float32))
    return (mixture / jnp.transpose(totals, (0, 2, 1))[..., None]).astype(jnp.bfloat16)

def row_attention(queries, key_heads, value_heads):
    total_rows = queries.shape[0]
    block_rows = math.gcd(total_rows, 1024)
    query_feat = jnp.transpose(queries, (1, 0, 2, 3)).reshape(F, total_rows // block_rows, block_rows, HEADS, HD)
    key_feat = jnp.transpose(key_heads, (1, 0, 2, 3))
    value_feat = jnp.transpose(value_heads, (1, 0, 2, 3))

    def one_feature(inputs):
        query_blocks, key_one, value_one = inputs
        key_float = key_one.astype(jnp.float32)
        value_float = value_one.astype(jnp.float32)

        def one_block(query_block):
            scores = jnp.einsum('qhd,khd->hqk', query_block.astype(jnp.float32), key_float) * HD ** (-0.5)
            row_peak = lax.optimization_barrier(jnp.max(scores, axis=-1, keepdims=True))
            weights = jnp.exp(scores - row_peak)
            totals = lax.optimization_barrier(jnp.sum(weights, axis=-1))
            mixture = jnp.einsum('hqk,khd->qhd', round_back(weights), value_float)
            return (mixture / jnp.transpose(totals)[..., None]).astype(jnp.bfloat16)
        return lax.map(one_block, query_blocks).reshape(total_rows, HEADS, HD)
    mixture = lax.map(one_feature, (query_feat, key_feat, value_feat))
    return jnp.transpose(mixture, (1, 0, 2, 3))

def reference(train_cells, test_cells, feat_weights, row_weights, mlp_up, mlp_down):
    joined = jnp.concatenate([train_cells, test_cells], axis=0)
    height = joined.shape[0]
    start_cells = joined.astype(jnp.float32).reshape(height, F, E)
    normed_one = layer_norm(start_cells).astype(jnp.bfloat16)
    feat_query = project(normed_one, feat_weights[0]).astype(jnp.bfloat16).reshape(height, F, HEADS, HD)
    feat_key = project(normed_one, feat_weights[1]).astype(jnp.bfloat16).reshape(height, F, HEADS, HD)
    feat_value = project(normed_one, feat_weights[2]).astype(jnp.bfloat16).reshape(height, F, HEADS, HD)
    feat_mix = feature_attention(feat_query, feat_key, feat_value)
    feat_out = project(feat_mix, feat_weights[3]).astype(jnp.bfloat16).reshape(height, F, E)
    after_feat = start_cells + feat_out.astype(jnp.float32)
    normed_two = layer_norm(after_feat).astype(jnp.bfloat16)
    row_query = project(normed_two, row_weights[0]).astype(jnp.bfloat16).reshape(height, F, HEADS, HD)
    train_normed = normed_two[:TRAIN]
    row_key = project(train_normed, row_weights[1]).astype(jnp.bfloat16).reshape(TRAIN, F, HEADS, HD)
    row_value = project(train_normed, row_weights[2]).astype(jnp.bfloat16).reshape(TRAIN, F, HEADS, HD)
    row_mix = row_attention(row_query, row_key, row_value)
    after_row = after_feat + project(row_mix, row_weights[3]).reshape(height, F, E)
    normed_three = layer_norm(after_row).astype(jnp.bfloat16)
    hidden = jax.nn.gelu(jnp.dot(normed_three.reshape(-1, E), mlp_up, preferred_element_type=jnp.float32), approximate=False).astype(jnp.bfloat16)
    lowered = jnp.dot(hidden, mlp_down, preferred_element_type=jnp.float32).reshape(height, F, E)
    result = (after_row + lowered).astype(jnp.bfloat16).reshape(height, F * E)
    return (result[:TRAIN], result[TRAIN:])
```

```python
import functools

import jax
import jax.numpy as jnp
from jax import lax
from jax.experimental import pallas as pl
from jax.experimental.pallas import tpu as pltpu
from jax.sharding import PartitionSpec as P

E = 192
HEADS = 6
HD = 32
HID = 768
F = 8
EPS = 1e-05
SCALE = HD ** (-0.5) * 1.4426950408889634
FAR = -1e30
MESH = pl.DeviceIdType.MESH
F32 = jnp.float32
BF16 = jnp.bfloat16

NX, NY, NZ, NC = 4, 4, 8, 2
TR, TE = 32, 16
RB = TR + TE
NQ = NZ * RB
KB = NZ * TR
HALF = KB // 2
STEPS = NX * NY

ORDER = [(0, 0), (1, 0), (2, 0), (0, 1), (0, 2), (3, 0), (1, 1), (2, 1),
         (1, 2), (2, 2), (0, 3), (3, 1), (3, 2), (1, 3), (2, 3), (3, 3)]
SLOT = {pos: i for i, pos in enumerate(ORDER)}


def nt(a, b):
    return lax.dot_general(a, b, (((1,), (1,)), ((), ())), preferred_element_type=F32)


def nn(a, b):
    return lax.dot_general(a, b, (((1,), (0,)), ((), ())), preferred_element_type=F32)


def norm(v):
    centred = v - jnp.mean(v, axis=-1, keepdims=True)
    spread = jnp.mean(centred * centred, axis=-1, keepdims=True)
    return centred * lax.rsqrt(spread + EPS)


def eye(n):
    r = lax.broadcasted_iota(jnp.int32, (n, n), 0)
    c = lax.broadcasted_iota(jnp.int32, (n, n), 1)
    return jnp.where(r == c, 1.0, 0.0).astype(BF16)


def head_mask(rows, h):
    lane = lax.broadcasted_iota(jnp.int32, (rows, E), 1)
    return (lane >= h * HD) & (lane < (h + 1) * HD)


def kernel(train_ref, test_ref, fw_ref, rw_ref, up_ref, down_ref,
           train_out, test_out,
           cell_tr, cell_te, x_ref, zs, zr, kbuf, qp, va, acc, mx, os_ref, or_ref, res,
           ex_send, ex_recv, z_send, z_recv, own_send, sib_send, ag_recv, ag_recv2, sib_recv,
           o_send, o_recv, loc):
    r = lax.axis_index("rows")
    h = lax.axis_index("feat")
    c = lax.rem(r, NC)
    z = lax.rem(r // NC, NZ)
    x = lax.rem(r // (NC * NZ), NX)
    ylo = r // (NC * NZ * NX)
    y = h * 2 + ylo

    def dev(x_, y_, z_, c_):
        row = ((lax.rem(y_, 2) * NX + x_) * NZ + z_) * NC + c_
        return {"rows": row, "feat": y_ // 2}

    first = jnp.where(c == 0, 1, 0)
    second = 1 - first

    def along(first_step, second_step):
        dx = first * first_step + second * second_step
        dy = second * first_step + first * second_step
        return dev(lax.rem(x + dx + NX, NX), lax.rem(y + dy + NY, NY), z, c)

    a_up, a_down = along(1, 0), along(-1, 0)
    b_up, b_down = along(0, 1), along(0, -1)
    sibling = dev(x, y, z, 1 - c)

    def z_line(d, other):
        return {"rows": ((ylo * NX + x) * NZ + lax.rem(z + d, NZ)) * NC + c,
                "feat": h if not other else 1 - h}

    barrier = pltpu.get_barrier_semaphore()
    for d in range(NZ):
        for other in (False, True):
            if d or other:
                pl.semaphore_signal(barrier, inc=1, device_id=z_line(d, other), device_id_type=MESH)
    for target in (a_up, a_down, b_up, b_down, sibling):
        pl.semaphore_signal(barrier, inc=1, device_id=target, device_id_type=MESH)
    pl.semaphore_wait(barrier, 2 * NZ - 1 + 5)

    def remote(src, dst, send, recv, target):
        return pltpu.make_async_remote_copy(src_ref=src, dst_ref=dst, send_sem=send, recv_sem=recv,
                                            device_id=target, device_id_type=MESH)

    partner = z_line(0, True)
    give_tr = pl.ds(pl.multiple_of((1 - h) * TR, TR), TR)
    give_te = pl.ds(pl.multiple_of((1 - h) * TE, TE), TE)
    ex = [remote(train_ref.at[give_tr], cell_tr.at[h], ex_send.at[0], ex_recv.at[0], partner),
          remote(test_ref.at[give_te], cell_te.at[h], ex_send.at[1], ex_recv.at[1], partner)]
    for copy in ex:
        copy.start()
    keep_tr = pl.ds(pl.multiple_of(h * TR, TR), TR)
    keep_te = pl.ds(pl.multiple_of(h * TE, TE), TE)
    cell_tr[h] = train_ref[keep_tr, :]
    cell_te[h] = test_ref[keep_te, :]
    for copy in ex:
        copy.wait()

    for f in range(F):
        lanes = slice((f % 4) * E, (f % 4 + 1) * E)
        for j in range(3):
            if j < 2:
                part = cell_tr[f // 4, 16 * j:16 * j + 16, lanes]
            else:
                part = cell_te[f // 4, :, lanes]
            x_ref[pl.ds(j * 128 + f * 16, 16), :] = part.astype(F32)
    cells = x_ref[...]
    n1 = norm(cells).astype(BF16)
    fq = nn(n1, fw_ref[0]).astype(BF16)
    fk = nn(n1, fw_ref[1]).astype(BF16)
    fv = nn(n1, fw_ref[2]).astype(BF16)
    same = (lax.rem(lax.broadcasted_iota(jnp.int32, (128, 128), 0), 16)
            == lax.rem(lax.broadcasted_iota(jnp.int32, (128, 128), 1), 16))
    zero = jnp.zeros((128, E), BF16)
    for j in range(3):
        rows = slice(128 * j, 128 * j + 128)
        qj, kj, vj = fq[rows], fk[rows], fv[rows]
        mixed = jnp.zeros((128, E), F32)
        for head in range(HEADS):
            mask = head_mask(128, head)
            s = nt(jnp.where(mask, qj, zero), kj) * SCALE
            s = jnp.where(same, s, FAR)
            w = jnp.exp2(s - jnp.max(s, axis=1, keepdims=True))
            total = jnp.sum(w, axis=1, keepdims=True)
            o = nn(w.astype(BF16), vj)
            mixed = jnp.where(mask, o / total, mixed)
        moved = nn(mixed.astype(BF16), fw_ref[3]).astype(BF16).astype(F32)
        after = (cells[rows] + moved).astype(BF16)
        for f in range(F):
            zs[f, 16 * j:16 * j + 16, :] = after[16 * f:16 * f + 16]

    z_copies = []
    for d in (4, 3, 5, 2, 6, 1, 7):
        copy = remote(zs.at[lax.rem(z + d, NZ)], zr.at[z], z_send.at[d], z_recv.at[d], z_line(d, False))
        copy.start()
        z_copies.append(copy)
    zr[z] = zs[z]
    for copy in z_copies:
        copy.wait_recv()

    a2 = zr[...].reshape(NQ, E).astype(F32)
    res[...] = a2
    n2 = norm(a2).astype(BF16)
    for k in range(NZ):
        kbuf[0, k * TR:(k + 1) * TR, :] = n2[k * RB:k * RB + TR]

    low, high = pl.ds(0, HALF), pl.ds(HALF, HALF)

    def send_block(slot, which, target, to_slot, rows, recv):
        src = kbuf.at[slot] if rows is None else kbuf.at[slot, rows]
        dst = kbuf.at[to_slot] if rows is None else kbuf.at[to_slot, rows]
        return remote(src, dst, own_send.at[slot, which], recv.at[to_slot], target)

    def sends(i):
        a, b = ORDER[i]
        out = []
        if (a, b) == (0, 0):
            out += [(0, a_up, SLOT[1, 0], None, ag_recv), (1, a_down, SLOT[2, 0], None, ag_recv)]
        if b == 0:
            out += [(2, b_up, SLOT[a, 1], None, ag_recv), (3, b_down, SLOT[a, 2], None, ag_recv)]
        if (a, b) == (1, 0):
            out += [(0, a_up, SLOT[3, 0], low, ag_recv)]
        if (a, b) == (2, 0):
            out += [(0, a_down, SLOT[3, 0], high, ag_recv2)]
        if b == 1:
            out += [(2, b_up, SLOT[a, 3], low, ag_recv)]
        if b == 2:
            out += [(2, b_down, SLOT[a, 3], high, ag_recv2)]
        return [send_block(i, *o) for o in out]

    def sib_copy(i):
        return remote(kbuf.at[i], kbuf.at[STEPS + i], sib_send.at[i], sib_recv.at[i], sibling)

    def handle(i):
        a, b = ORDER[i]
        if i:
            if a == 3 and b == 0 or b == 3:
                remote(kbuf.at[i, low], kbuf.at[i, low], own_send.at[i, 0], ag_recv.at[i], a_up).wait_recv()
                remote(kbuf.at[i, high], kbuf.at[i, high], own_send.at[i, 0], ag_recv2.at[i], a_up).wait_recv()
            else:
                remote(kbuf.at[i], kbuf.at[i], own_send.at[i, 0], ag_recv.at[i], a_up).wait_recv()
        for copy in sends(i):
            copy.start()
        sib_copy(i).start()

    handle(0)

    q2 = nn(n2, rw_ref[0]).astype(BF16)
    wk = rw_ref[1]
    zero = jnp.zeros((E, E), BF16)
    for head in range(HEADS):
        part = nt(jnp.where(head_mask(E, head), wk, zero), q2) * SCALE
        qp[head // 2, :, (head % 2) * NQ:(head % 2 + 1) * NQ] = part.astype(BF16)
    wvt = nt(eye(E), rw_ref[2]).astype(BF16)
    va[...] = jnp.ones_like(va)
    acc[...] = jnp.zeros_like(acc)
    mx[...] = jnp.full_like(mx, FAR)

    def step(i, carry):
        for k in range(1, STEPS):
            @pl.when(i == k - 1)
            def _():
                handle(k)
        remote(kbuf.at[0], kbuf.at[STEPS + i], sib_send.at[i], sib_recv.at[i], sibling).wait_recv()
        keys = jnp.concatenate([kbuf[i], kbuf[STEPS + i]], axis=0)
        vt = nt(wvt, keys).astype(BF16)
        for g in range(3):
            va[g, 0:64, :] = vt[64 * g:64 * g + 64]
        for g in range(3):
            s = nn(keys, qp[g])
            old = mx[g]
            new = jnp.maximum(old, jnp.max(s, axis=0, keepdims=True))
            mx[g] = new
            w = jnp.exp2(s - new).astype(BF16)
            acc[g] = acc[g] * jnp.exp2(old - new) + nn(va[g], w)
        return carry

    lax.fori_loop(0, STEPS, step, 0)

    parts = []
    for g in range(3):
        o = acc[g]
        o = o[0:64] / o[64:65]
        parts += [o[0:32, 0:NQ], o[32:64, NQ:2 * NQ]]
    mix_t = jnp.concatenate(parts, axis=0).astype(BF16)
    mix = nt(eye(NQ), mix_t).astype(BF16)
    after_row = res[...] + nn(mix, rw_ref[3])
    n3 = norm(after_row).astype(BF16)
    hidden = nn(n3, up_ref[...])
    hidden = (hidden * 0.5 * (1.0 + lax.erf(hidden * (2.0 ** -0.5)))).astype(BF16)
    out = (after_row + nn(hidden, down_ref[...])).astype(BF16)
    for k in range(NZ):
        os_ref[k] = out[k * RB:(k + 1) * RB]

    side = z // 4
    mine = lax.rem(z, 4)

    def out_copy(d):
        target = {"rows": ((ylo * NX + x) * NZ + lax.rem(z + d, NZ)) * NC + c, "feat": side}
        return remote(os_ref.at[lax.rem(z + d, NZ)], or_ref.at[mine, h], o_send.at[d], o_recv.at[mine, h], target)

    for d in (4, 3, 5, 2, 6, 1, 7):
        out_copy(d).start()

    @pl.when(side == h)
    def _():
        or_ref[mine, h] = os_ref[z]

    @pl.when(side != h)
    def _():
        out_copy(0).start()

    for i in range(4):
        for hs in range(2):
            own = (side == h) & (mine == i) & (h == hs)

            @pl.when(jnp.logical_not(own))
            def _():
                remote(os_ref.at[0], or_ref.at[i, hs], o_send.at[0], o_recv.at[i, hs], partner).wait_recv()

    for hs in range(2):
        blocks = [or_ref[i, hs] for i in range(4)]
        train_out[TR * hs:TR * hs + TR, :] = jnp.concatenate([b[0:TR] for b in blocks], axis=1)
        test_out[TE * hs:TE * hs + TE, :] = jnp.concatenate([b[TR:RB] for b in blocks], axis=1)

    for copy in z_copies:
        copy.wait_send()
    for i in range(STEPS):
        for copy in sends(i):
            copy.wait_send()
        sib_copy(i).wait_send()
    for d in range(1, NZ):
        out_copy(d).wait_send()

    @pl.when(side != h)
    def _():
        out_copy(0).wait_send()


def body(*args):
    train, test = args[0], args[1]
    dma = pltpu.SemaphoreType.DMA
    return pl.pallas_call(
        kernel,
        name="layer",
        out_shape=(jax.ShapeDtypeStruct(train.shape, BF16), jax.ShapeDtypeStruct(test.shape, BF16)),
        in_specs=[pl.BlockSpec(memory_space=pltpu.VMEM)] * 6,
        out_specs=(pl.BlockSpec(memory_space=pltpu.VMEM),) * 2,
        scratch_shapes=[
            pltpu.VMEM((2, TR, 4 * E), BF16),
            pltpu.VMEM((2, TE, 4 * E), BF16),
            pltpu.VMEM((NQ, E), F32),
            pltpu.VMEM((F, RB, E), BF16),
            pltpu.VMEM((NZ, RB, E), BF16),
            pltpu.VMEM((2 * STEPS, KB, E), BF16),
            pltpu.VMEM((3, E, 2 * NQ), BF16),
            pltpu.VMEM((3, 80, 2 * KB), BF16),
            pltpu.VMEM((3, 80, 2 * NQ), F32),
            pltpu.VMEM((3, 1, 2 * NQ), F32),
            pltpu.VMEM((NZ, RB, E), BF16),
            pltpu.VMEM((4, 2, RB, E), BF16),
            pltpu.VMEM((NQ, E), F32),
            dma((2,)), dma((2,)), dma((NZ,)), dma((NZ,)),
            dma((STEPS, 4)), dma((STEPS,)), dma((STEPS,)), dma((STEPS,)), dma((STEPS,)),
            dma((NZ,)), dma((4, 2)), dma((1,)),
        ],
        compiler_params=pltpu.CompilerParams(
            collective_id=0, has_side_effects=True, vmem_limit_bytes=60 * 1024 * 1024),
    )(*args)


def solution(mesh):
    return jax.shard_map(
        body,
        mesh=mesh,
        in_specs=(P("rows", "feat"), P("rows", "feat"), P(), P(), P(), P()),
        out_specs=(P("rows", "feat"), P("rows", "feat")),
        check_vma=False,
    )
```

```python
import functools

import jax
import jax.numpy as jnp
from jax import lax
from jax.experimental import pallas as pl
from jax.experimental.pallas import tpu as pltpu
from jax.sharding import PartitionSpec as P

E = 192
HEADS = 6
HD = 32
HID = 768
F = 8
EPS = 1e-05
SCALE = HD ** (-0.5) * 1.4426950408889634
FAR = -1e30
MESH = pl.DeviceIdType.MESH
F32 = jnp.float32
BF16 = jnp.bfloat16

NX, NY, NZ, NC = 4, 4, 8, 2
TR, TE = 32, 16
RB = TR + TE
NQ = NZ * RB
KB = NZ * TR
HALF = KB // 2
STEPS = NX * NY
UW = 256
UNITS = HEADS * NQ // UW

ORDER = [(0, 0), (1, 0), (2, 0), (0, 1), (0, 2), (3, 0), (1, 1), (2, 1),
         (1, 2), (2, 2), (0, 3), (3, 1), (3, 2), (1, 3), (2, 3), (3, 3)]
SLOT = {pos: i for i, pos in enumerate(ORDER)}


def nt(a, b):
    return lax.dot_general(a, b, (((1,), (1,)), ((), ())), preferred_element_type=F32)


def nn(a, b):
    return lax.dot_general(a, b, (((1,), (0,)), ((), ())), preferred_element_type=F32)


def norm(v):
    centred = v - jnp.mean(v, axis=-1, keepdims=True)
    spread = jnp.mean(centred * centred, axis=-1, keepdims=True)
    return centred * lax.rsqrt(spread + EPS)


def eye(n):
    r = lax.broadcasted_iota(jnp.int32, (n, n), 0)
    c = lax.broadcasted_iota(jnp.int32, (n, n), 1)
    return jnp.where(r == c, 1.0, 0.0).astype(BF16)


def head_mask(rows, h):
    lane = lax.broadcasted_iota(jnp.int32, (rows, E), 1)
    return (lane >= h * HD) & (lane < (h + 1) * HD)


def kernel(train_ref, test_ref, fw_ref, rw_ref, up_ref, down_ref,
           train_out, test_out,
           cell_tr, cell_te, x_ref, zs, zr, kbuf, qp, va, sbuf, acc, m_acc, m_new, os_ref, or_ref, res,
           ex_send, ex_recv, z_send, z_recv, own_send, sib_send, ag_recv, ag_recv2, sib_recv,
           o_send, o_recv, loc):
    r = lax.axis_index("rows")
    h = lax.axis_index("feat")
    c = lax.rem(r, NC)
    z = lax.rem(r // NC, NZ)
    x = lax.rem(r // (NC * NZ), NX)
    ylo = r // (NC * NZ * NX)
    y = h * 2 + ylo

    def dev(x_, y_, z_, c_):
        row = ((lax.rem(y_, 2) * NX + x_) * NZ + z_) * NC + c_
        return {"rows": row, "feat": y_ // 2}

    first = jnp.where(c == 0, 1, 0)
    second = 1 - first

    def along(first_step, second_step):
        dx = first * first_step + second * second_step
        dy = second * first_step + first * second_step
        return dev(lax.rem(x + dx + NX, NX), lax.rem(y + dy + NY, NY), z, c)

    a_up, a_down = along(1, 0), along(-1, 0)
    b_up, b_down = along(0, 1), along(0, -1)
    sibling = dev(x, y, z, 1 - c)

    def z_line(d, other):
        return {"rows": ((ylo * NX + x) * NZ + lax.rem(z + d, NZ)) * NC + c,
                "feat": h if not other else 1 - h}

    barrier = pltpu.get_barrier_semaphore()
    for d in range(NZ):
        for other in (False, True):
            if d or other:
                pl.semaphore_signal(barrier, inc=1, device_id=z_line(d, other), device_id_type=MESH)
    for target in (a_up, a_down, b_up, b_down, sibling):
        pl.semaphore_signal(barrier, inc=1, device_id=target, device_id_type=MESH)
    pl.semaphore_wait(barrier, 2 * NZ - 1 + 5)

    def remote(src, dst, send, recv, target):
        return pltpu.make_async_remote_copy(src_ref=src, dst_ref=dst, send_sem=send, recv_sem=recv,
                                            device_id=target, device_id_type=MESH)

    partner = z_line(0, True)
    give_tr = pl.ds(pl.multiple_of((1 - h) * TR, TR), TR)
    give_te = pl.ds(pl.multiple_of((1 - h) * TE, TE), TE)
    ex = [remote(train_ref.at[give_tr], cell_tr.at[h], ex_send.at[0], ex_recv.at[0], partner),
          remote(test_ref.at[give_te], cell_te.at[h], ex_send.at[1], ex_recv.at[1], partner)]
    for copy in ex:
        copy.start()
    keep_tr = pl.ds(pl.multiple_of(h * TR, TR), TR)
    keep_te = pl.ds(pl.multiple_of(h * TE, TE), TE)
    cell_tr[h] = train_ref[keep_tr, :]
    cell_te[h] = test_ref[keep_te, :]
    for copy in ex:
        copy.wait()

    for f in range(F):
        lanes = slice((f % 4) * E, (f % 4 + 1) * E)
        for j in range(3):
            if j < 2:
                part = cell_tr[f // 4, 16 * j:16 * j + 16, lanes]
            else:
                part = cell_te[f // 4, :, lanes]
            x_ref[pl.ds(j * 128 + f * 16, 16), :] = part.astype(F32)
    cells = x_ref[...]
    n1 = norm(cells).astype(BF16)
    fq = nn(n1, fw_ref[0]).astype(BF16)
    fk = nn(n1, fw_ref[1]).astype(BF16)
    fv = nn(n1, fw_ref[2]).astype(BF16)
    same = (lax.rem(lax.broadcasted_iota(jnp.int32, (128, 128), 0), 16)
            == lax.rem(lax.broadcasted_iota(jnp.int32, (128, 128), 1), 16))
    zero = jnp.zeros((128, E), BF16)
    for j in range(3):
        rows = slice(128 * j, 128 * j + 128)
        qj, kj, vj = fq[rows], fk[rows], fv[rows]
        mixed = jnp.zeros((128, E), F32)
        for head in range(HEADS):
            mask = head_mask(128, head)
            s = nt(jnp.where(mask, qj, zero), kj) * SCALE
            s = jnp.where(same, s, FAR)
            w = jnp.exp2(s - jnp.max(s, axis=1, keepdims=True))
            total = jnp.sum(w, axis=1, keepdims=True)
            o = nn(w.astype(BF16), vj)
            mixed = jnp.where(mask, o / total, mixed)
        moved = nn(mixed.astype(BF16), fw_ref[3]).astype(BF16).astype(F32)
        after = (cells[rows] + moved).astype(BF16)
        for f in range(F):
            zs[f, 16 * j:16 * j + 16, :] = after[16 * f:16 * f + 16]

    z_copies = []
    for d in (4, 3, 5, 2, 6, 1, 7):
        copy = remote(zs.at[lax.rem(z + d, NZ)], zr.at[z], z_send.at[d], z_recv.at[d], z_line(d, False))
        copy.start()
        z_copies.append(copy)
    zr[z] = zs[z]
    for copy in z_copies:
        copy.wait_recv()

    a2 = zr[...].reshape(NQ, E).astype(F32)
    res[...] = a2
    n2 = norm(a2).astype(BF16)
    for k in range(NZ):
        kbuf[0, k * TR:(k + 1) * TR, :] = n2[k * RB:k * RB + TR]

    low, high = pl.ds(0, HALF), pl.ds(HALF, HALF)

    def send_block(slot, which, target, to_slot, rows, recv):
        src = kbuf.at[slot] if rows is None else kbuf.at[slot, rows]
        dst = kbuf.at[to_slot] if rows is None else kbuf.at[to_slot, rows]
        return remote(src, dst, own_send.at[slot, which], recv.at[to_slot], target)

    def sends(i):
        a, b = ORDER[i]
        out = []
        if (a, b) == (0, 0):
            out += [(0, a_up, SLOT[1, 0], None, ag_recv), (1, a_down, SLOT[2, 0], None, ag_recv)]
        if b == 0:
            out += [(2, b_up, SLOT[a, 1], None, ag_recv), (3, b_down, SLOT[a, 2], None, ag_recv)]
        if (a, b) == (1, 0):
            out += [(0, a_up, SLOT[3, 0], low, ag_recv)]
        if (a, b) == (2, 0):
            out += [(0, a_down, SLOT[3, 0], high, ag_recv2)]
        if b == 1:
            out += [(2, b_up, SLOT[a, 3], low, ag_recv)]
        if b == 2:
            out += [(2, b_down, SLOT[a, 3], high, ag_recv2)]
        return [send_block(i, *o) for o in out]

    def sib_copy(i):
        return remote(kbuf.at[i], kbuf.at[STEPS + i], sib_send.at[i], sib_recv.at[i], sibling)

    def handle(i):
        a, b = ORDER[i]
        if i:
            if a == 3 and b == 0 or b == 3:
                remote(kbuf.at[i, low], kbuf.at[i, low], own_send.at[i, 0], ag_recv.at[i], a_up).wait_recv()
                remote(kbuf.at[i, high], kbuf.at[i, high], own_send.at[i, 0], ag_recv2.at[i], a_up).wait_recv()
            else:
                remote(kbuf.at[i], kbuf.at[i], own_send.at[i, 0], ag_recv.at[i], a_up).wait_recv()
        for copy in sends(i):
            copy.start()
        sib_copy(i).start()

    handle(0)

    q2 = nn(n2, rw_ref[0]).astype(BF16)
    wk = rw_ref[1]
    zero = jnp.zeros((E, E), BF16)
    for g in range(HEADS // 2):
        pair = [(nt(jnp.where(head_mask(E, 2 * g + k), wk, zero), q2) * SCALE).astype(BF16) for k in range(2)]
        pair = jnp.concatenate(pair, axis=1)
        for t in range(3):
            qp[3 * g + t] = pair[:, UW * t:UW * t + UW]
    wvt = nt(eye(E), rw_ref[2]).astype(BF16)
    va[...] = jnp.ones_like(va)
    acc[...] = jnp.zeros_like(acc)
    m_acc[...] = jnp.full_like(m_acc, FAR)
    m_new[...] = jnp.full_like(m_new, FAR)

    span = [(0, 48), (0, 80), (32, 80)]

    def score(i, u):
        for k in range(2):
            s = nn(kbuf[i + STEPS * k], qp[u])
            sbuf[u % 3, KB * k:KB * k + KB, :] = s
            m_new[u] = jnp.maximum(m_new[u], jnp.max(s, axis=0, keepdims=True))

    def weigh(u):
        lo, hi = span[u % 3]
        new = m_new[u]
        fade = jnp.exp2(m_acc[u] - new)
        m_acc[u] = new
        w = jnp.exp2(sbuf[u % 3] - new).astype(BF16)
        acc[u, lo:hi, :] = acc[u, lo:hi, :] * fade + nn(va[u // 3, lo:hi, :], w)

    def values(i):
        for k in range(2):
            vt = nt(wvt, kbuf[i + STEPS * k]).astype(BF16)
            for g in range(3):
                va[g, 0:32, KB * k:KB * k + KB] = vt[64 * g:64 * g + 32]
                va[g, 48:80, KB * k:KB * k + KB] = vt[64 * g + 32:64 * g + 64]

    def arrive(i):
        remote(kbuf.at[0], kbuf.at[STEPS + i], sib_send.at[i], sib_recv.at[i], sibling).wait_recv()

    def advance(i, following):
        values(i)
        for u in range(UNITS):
            if u + 1 < UNITS:
                score(i, u + 1)
            elif following is not None:
                score(following, 0)
            weigh(u)

    arrive(0)
    score(0, 0)
    advance(0, None)
    handle(1)
    arrive(1)
    score(1, 0)

    def step(i, carry):
        for k in range(2, STEPS):
            @pl.when(i == k - 1)
            def _():
                handle(k)

        @pl.when(i < STEPS - 1)
        def _():
            arrive(i + 1)

        advance(i, jnp.minimum(i + 1, STEPS - 1))
        return carry

    lax.fori_loop(1, STEPS, step, 0)

    parts = []
    for g in range(3):
        o = [acc[3 * g + t] for t in range(3)]
        o = [v / v[32:33] for v in o]
        parts += [jnp.concatenate([o[0][0:32], o[1][0:32, 0:UW // 2]], axis=1),
                  jnp.concatenate([o[1][48:80, UW // 2:], o[2][48:80]], axis=1)]
    mix_t = jnp.concatenate(parts, axis=0).astype(BF16)
    mix = nt(eye(NQ), mix_t).astype(BF16)
    after_row = res[...] + nn(mix, rw_ref[3])
    n3 = norm(after_row).astype(BF16)
    hidden = nn(n3, up_ref[...])
    hidden = (hidden * 0.5 * (1.0 + lax.erf(hidden * (2.0 ** -0.5)))).astype(BF16)
    out = (after_row + nt(hidden, down_ref[...])).astype(BF16)
    for k in range(NZ):
        os_ref[k] = out[k * RB:(k + 1) * RB]

    side = z // 4
    mine = lax.rem(z, 4)

    def out_copy(d):
        target = {"rows": ((ylo * NX + x) * NZ + lax.rem(z + d, NZ)) * NC + c, "feat": side}
        return remote(os_ref.at[lax.rem(z + d, NZ)], or_ref.at[mine, h], o_send.at[d], o_recv.at[mine, h], target)

    for d in (4, 3, 5, 2, 6, 1, 7):
        out_copy(d).start()

    @pl.when(side == h)
    def _():
        or_ref[mine, h] = os_ref[z]

    @pl.when(side != h)
    def _():
        out_copy(0).start()

    for i in range(4):
        for hs in range(2):
            own = (side == h) & (mine == i) & (h == hs)

            @pl.when(jnp.logical_not(own))
            def _():
                remote(os_ref.at[0], or_ref.at[i, hs], o_send.at[0], o_recv.at[i, hs], partner).wait_recv()

    for hs in range(2):
        blocks = [or_ref[i, hs] for i in range(4)]
        train_out[TR * hs:TR * hs + TR, :] = jnp.concatenate([b[0:TR] for b in blocks], axis=1)
        test_out[TE * hs:TE * hs + TE, :] = jnp.concatenate([b[TR:RB] for b in blocks], axis=1)

    for copy in z_copies:
        copy.wait_send()
    for i in range(STEPS):
        for copy in sends(i):
            copy.wait_send()
        sib_copy(i).wait_send()
    for d in range(1, NZ):
        out_copy(d).wait_send()

    @pl.when(side != h)
    def _():
        out_copy(0).wait_send()


def body(*args):
    train, test = args[0], args[1]
    dma = pltpu.SemaphoreType.DMA
    return pl.pallas_call(
        kernel,
        name="layer",
        out_shape=(jax.ShapeDtypeStruct(train.shape, BF16), jax.ShapeDtypeStruct(test.shape, BF16)),
        in_specs=[pl.BlockSpec(memory_space=pltpu.VMEM)] * 6,
        out_specs=(pl.BlockSpec(memory_space=pltpu.VMEM),) * 2,
        scratch_shapes=[
            pltpu.VMEM((2, TR, 4 * E), BF16),
            pltpu.VMEM((2, TE, 4 * E), BF16),
            pltpu.VMEM((NQ, E), F32),
            pltpu.VMEM((F, RB, E), BF16),
            pltpu.VMEM((NZ, RB, E), BF16),
            pltpu.VMEM((2 * STEPS, KB, E), BF16),
            pltpu.VMEM((UNITS, E, UW), BF16),
            pltpu.VMEM((3, 80, 2 * KB), BF16),
            pltpu.VMEM((3, 2 * KB, UW), F32),
            pltpu.VMEM((UNITS, 80, UW), F32),
            pltpu.VMEM((UNITS, 1, UW), F32),
            pltpu.VMEM((UNITS, 1, UW), F32),
            pltpu.VMEM((NZ, RB, E), BF16),
            pltpu.VMEM((4, 2, RB, E), BF16),
            pltpu.VMEM((NQ, E), F32),
            dma((2,)), dma((2,)), dma((NZ,)), dma((NZ,)),
            dma((STEPS, 4)), dma((STEPS,)), dma((STEPS,)), dma((STEPS,)), dma((STEPS,)),
            dma((NZ,)), dma((4, 2)), dma((1,)),
        ],
        compiler_params=pltpu.CompilerParams(
            collective_id=0, has_side_effects=True, vmem_limit_bytes=60 * 1024 * 1024),
    )(*args[:5], args[5].T)


def solution(mesh):
    return jax.shard_map(
        body,
        mesh=mesh,
        in_specs=(P("rows", "feat"), P("rows", "feat"), P(), P(), P(), P()),
        out_specs=(P("rows", "feat"), P("rows", "feat")),
        check_vma=False,
    )
```

```python
import functools

import jax
import jax.numpy as jnp
from jax import lax
from jax.experimental import pallas as pl
from jax.experimental.pallas import tpu as pltpu
from jax.sharding import PartitionSpec as P

E = 192
HEADS = 6
HD = 32
HID = 768
F = 8
EPS = 1e-05
SCALE = HD ** (-0.5) * 1.4426950408889634
FAR = -1e30
MESH = pl.DeviceIdType.MESH
F32 = jnp.float32
BF16 = jnp.bfloat16

NX, NY, NZ, NC = 4, 4, 8, 2
TR, TE = 32, 16
RB = TR + TE
NQ = NZ * RB
KB = NZ * TR
BLOCK = KB * 3 // 2
HALF = BLOCK // 2
ZB = RB + 2 * TE
STEPS = NX * NY
UW = 256
UNITS = HEADS * NQ // UW

ORDER = [(0, 0), (1, 0), (2, 0), (0, 1), (0, 2), (3, 0), (1, 1), (2, 1),
         (1, 2), (2, 2), (0, 3), (3, 1), (3, 2), (1, 3), (2, 3), (3, 3)]
SLOT = {pos: i for i, pos in enumerate(ORDER)}


def nt(a, b):
    return lax.dot_general(a, b, (((1,), (1,)), ((), ())), preferred_element_type=F32)


def nn(a, b):
    return lax.dot_general(a, b, (((1,), (0,)), ((), ())), preferred_element_type=F32)


def norm(v):
    centred = v - jnp.mean(v, axis=-1, keepdims=True)
    spread = jnp.mean(centred * centred, axis=-1, keepdims=True)
    return centred * lax.rsqrt(spread + EPS)


def eye(n):
    r = lax.broadcasted_iota(jnp.int32, (n, n), 0)
    c = lax.broadcasted_iota(jnp.int32, (n, n), 1)
    return jnp.where(r == c, 1.0, 0.0).astype(BF16)


def head_mask(rows, h):
    lane = lax.broadcasted_iota(jnp.int32, (rows, E), 1)
    return (lane >= h * HD) & (lane < (h + 1) * HD)


def kernel(train_in, test_in, fw_in, rw_in, up_in, down_in,
           train_out, test_out,
           train_ref, test_ref, fw_ref, rw_ref, up_ref, down_ref,
           cell_tr, cell_te, x_ref, zs, zr, kbuf, qp, wv, va, sbuf, acc, m_acc, m_new, os_ref, or_ref, res,
           ex_send, ex_recv, z_send, z_recv, own_send, sib_send, ag_recv, ag_recv2, sib_recv,
           o_send, o_recv, in_sem):
    r = lax.axis_index("rows")
    h = lax.axis_index("feat")
    c = lax.rem(r, NC)
    z = lax.rem(r // NC, NZ)
    x = lax.rem(r // (NC * NZ), NX)
    ylo = r // (NC * NZ * NX)
    y = h * 2 + ylo

    def dev(x_, y_, z_, c_):
        row = ((lax.rem(y_, 2) * NX + x_) * NZ + z_) * NC + c_
        return {"rows": row, "feat": y_ // 2}

    first = jnp.where(c == 0, 1, 0)
    second = 1 - first

    def along(first_step, second_step):
        dx = first * first_step + second * second_step
        dy = second * first_step + first * second_step
        return dev(lax.rem(x + dx + NX, NX), lax.rem(y + dy + NY, NY), z, c)

    a_up, a_down = along(1, 0), along(-1, 0)
    b_up, b_down = along(0, 1), along(0, -1)
    sibling = dev(x, y, z, 1 - c)

    def z_line(d, other):
        return {"rows": ((ylo * NX + x) * NZ + lax.rem(z + d, NZ)) * NC + c,
                "feat": h if not other else 1 - h}

    barrier = pltpu.get_barrier_semaphore()
    for d in range(NZ):
        for other in (False, True):
            if d or other:
                pl.semaphore_signal(barrier, inc=1, device_id=z_line(d, other), device_id_type=MESH)
    for target in (a_up, a_down, b_up, b_down, sibling):
        pl.semaphore_signal(barrier, inc=1, device_id=target, device_id_type=MESH)
    fetch = [pltpu.make_async_copy(a, b, in_sem.at[k]) for k, (a, b) in enumerate((
        (train_in, train_ref), (test_in, test_ref), (fw_in, fw_ref), (rw_in, rw_ref),
        (up_in, up_ref), (down_in, down_ref)))]
    for copy in fetch:
        copy.start()
    fetch[0].wait()
    fetch[1].wait()
    pl.semaphore_wait(barrier, 2 * NZ - 1 + 5)

    def remote(src, dst, send, recv, target):
        return pltpu.make_async_remote_copy(src_ref=src, dst_ref=dst, send_sem=send, recv_sem=recv,
                                            device_id=target, device_id_type=MESH)

    partner = z_line(0, True)
    give_tr = pl.ds(pl.multiple_of((1 - h) * TR, TR), TR)
    give_te = pl.ds(pl.multiple_of((1 - h) * TE, TE), TE)
    ex = [remote(train_ref.at[give_tr], cell_tr.at[h], ex_send.at[0], ex_recv.at[0], partner),
          remote(test_ref.at[give_te], cell_te.at[h], ex_send.at[1], ex_recv.at[1], partner)]
    for copy in ex:
        copy.start()
    keep_tr = pl.ds(pl.multiple_of(h * TR, TR), TR)
    keep_te = pl.ds(pl.multiple_of(h * TE, TE), TE)
    cell_tr[h] = train_ref[keep_tr, :]
    cell_te[h] = test_ref[keep_te, :]
    fetch[2].wait()
    for copy in ex:
        copy.wait()

    for f in range(F):
        lanes = slice((f % 4) * E, (f % 4 + 1) * E)
        for j in range(3):
            if j < 2:
                part = cell_tr[f // 4, 16 * j:16 * j + 16, lanes]
            else:
                part = cell_te[f // 4, :, lanes]
            x_ref[pl.ds(j * 128 + f * 16, 16), :] = part.astype(F32)
    cells = x_ref[...]
    n1 = norm(cells).astype(BF16)
    fq = nn(n1, fw_ref[0]).astype(BF16)
    fk = nn(n1, fw_ref[1]).astype(BF16)
    fv = nn(n1, fw_ref[2]).astype(BF16)
    same = (lax.rem(lax.broadcasted_iota(jnp.int32, (128, 128), 0), 16)
            == lax.rem(lax.broadcasted_iota(jnp.int32, (128, 128), 1), 16))
    zero = jnp.zeros((128, E), BF16)
    rest = []
    for j in range(3):
        rows = slice(128 * j, 128 * j + 128)
        qj, kj, vj = fq[rows], fk[rows], fv[rows]
        mixed = jnp.zeros((128, E), F32)
        for head in range(HEADS):
            mask = head_mask(128, head)
            s = nt(jnp.where(mask, qj, zero), kj) * SCALE
            s = jnp.where(same, s, FAR)
            w = jnp.exp2(s - jnp.max(s, axis=1, keepdims=True))
            total = jnp.sum(w, axis=1, keepdims=True)
            o = nn(w.astype(BF16), vj)
            mixed = jnp.where(mask, o / total, mixed)
        moved = nn(mixed.astype(BF16), fw_ref[3]).astype(BF16).astype(F32)
        after = (cells[rows] + moved).astype(BF16)
        for f in range(F):
            zs[f, 16 * j:16 * j + 16, :] = after[16 * f:16 * f + 16, 0:128]
        rest.append(after[:, 128:E])
    for f in range(F):
        own = slice(16 * f, 16 * f + 16)
        zs[f, RB:RB + TE, :] = jnp.concatenate([rest[0][own], rest[1][own]], axis=1)
        zs[f, RB + TE:ZB, :] = jnp.concatenate([rest[2][own], rest[2][own]], axis=1)

    z_copies = []
    for d in (4, 3, 5, 2, 6, 1, 7):
        copy = remote(zs.at[lax.rem(z + d, NZ)], zr.at[z], z_send.at[d], z_recv.at[d], z_line(d, False))
        copy.start()
        z_copies.append(copy)
    zr[z] = zs[z]
    for copy in z_copies:
        copy.wait_recv()

    for k in range(NZ):
        left = zr[k, 0:RB, :]
        pair = zr[k, RB:RB + TE, :]
        right = jnp.concatenate([pair[:, 0:64], pair[:, 64:128], zr[k, RB + TE:ZB, 0:64]], axis=0)
        res[k * RB:(k + 1) * RB, :] = jnp.concatenate([left, right], axis=1).astype(F32)
    n2 = norm(res[...]).astype(BF16)
    keys = jnp.concatenate([n2[k * RB:k * RB + TR] for k in range(NZ)], axis=0)
    kbuf[0, 0:KB, :] = keys[:, 0:128]
    kbuf[0, KB:BLOCK, :] = jnp.concatenate([keys[0:KB // 2, 128:E], keys[KB // 2:KB, 128:E]], axis=1)

    low, high = pl.ds(0, HALF), pl.ds(HALF, HALF)

    def send_block(slot, which, target, to_slot, rows, recv):
        src = kbuf.at[slot] if rows is None else kbuf.at[slot, rows]
        dst = kbuf.at[to_slot] if rows is None else kbuf.at[to_slot, rows]
        return remote(src, dst, own_send.at[slot, which], recv.at[to_slot], target)

    def sends(i):
        a, b = ORDER[i]
        out = []
        if (a, b) == (0, 0):
            out += [(0, a_up, SLOT[1, 0], None, ag_recv), (1, a_down, SLOT[2, 0], None, ag_recv)]
        if b == 0:
            out += [(2, b_up, SLOT[a, 1], None, ag_recv), (3, b_down, SLOT[a, 2], None, ag_recv)]
        if (a, b) == (1, 0):
            out += [(0, a_up, SLOT[3, 0], low, ag_recv)]
        if (a, b) == (2, 0):
            out += [(0, a_down, SLOT[3, 0], high, ag_recv2)]
        if b == 1:
            out += [(2, b_up, SLOT[a, 3], low, ag_recv)]
        if b == 2:
            out += [(2, b_down, SLOT[a, 3], high, ag_recv2)]
        return [send_block(i, *o) for o in out]

    def sib_copy(i):
        return remote(kbuf.at[i], kbuf.at[STEPS + i], sib_send.at[i], sib_recv.at[i], sibling)

    def handle(i):
        a, b = ORDER[i]
        if i:
            if a == 3 and b == 0 or b == 3:
                remote(kbuf.at[i, low], kbuf.at[i, low], own_send.at[i, 0], ag_recv.at[i], a_up).wait_recv()
                remote(kbuf.at[i, high], kbuf.at[i, high], own_send.at[i, 0], ag_recv2.at[i], a_up).wait_recv()
            else:
                remote(kbuf.at[i], kbuf.at[i], own_send.at[i, 0], ag_recv.at[i], a_up).wait_recv()
        for copy in sends(i):
            copy.start()
        sib_copy(i).start()

    handle(0)

    fetch[3].wait()
    fetch[4].wait()
    fetch[5].wait()
    q2 = nn(n2, rw_ref[0]).astype(BF16)
    wk = rw_ref[1]
    zero = jnp.zeros((E, E), BF16)
    for g in range(HEADS // 2):
        pair = [(nt(jnp.where(head_mask(E, 2 * g + k), wk, zero), q2) * SCALE).astype(BF16) for k in range(2)]
        pair = jnp.concatenate(pair, axis=1)
        for t in range(3):
            part = pair[:, UW * t:UW * t + UW]
            for k in range(2):
                qp[3 * g + t, k, 0:128, :] = part[0:128]
                qp[3 * g + t, k, 128 + 64 * k:192 + 64 * k, :] = part[128:E]
                qp[3 * g + t, k, 192 - 64 * k:256 - 64 * k, :] = jnp.zeros((64, UW), BF16)
    wvt = nt(eye(E), rw_ref[2]).astype(BF16)
    gap = jnp.zeros((E, 64), BF16)
    wv[0] = jnp.concatenate([wvt, gap], axis=1)
    wv[1] = jnp.concatenate([wvt[:, 0:128], gap, wvt[:, 128:E]], axis=1)
    va[...] = jnp.ones_like(va)
    acc[...] = jnp.zeros_like(acc)
    m_acc[...] = jnp.full_like(m_acc, FAR)
    m_new[...] = jnp.full_like(m_new, FAR)

    span = [(0, 48), (0, 80), (32, 80)]

    def half_keys(i, k):
        return jnp.concatenate([
            jnp.concatenate([kbuf[i + STEPS * p, 128 * k:128 * k + 128, :], kbuf[i + STEPS * p, KB:BLOCK, :]], axis=1)
            for p in range(2)], axis=0)

    def score(i, u):
        for k in range(2):
            s = nn(half_keys(i, k), qp[u, k])
            sbuf[u % 3, KB * k:KB * k + KB, :] = s
            m_new[u] = jnp.maximum(m_new[u], jnp.max(s, axis=0, keepdims=True))

    def weigh(u):
        lo, hi = span[u % 3]
        new = m_new[u]
        fade = jnp.exp2(m_acc[u] - new)
        m_acc[u] = new
        w = jnp.exp2(sbuf[u % 3] - new).astype(BF16)
        acc[u, lo:hi, :] = acc[u, lo:hi, :] * fade + nn(va[u // 3, lo:hi, :], w)

    def values(i):
        for k in range(2):
            vt = nt(wv[k], half_keys(i, k)).astype(BF16)
            for g in range(3):
                va[g, 0:32, KB * k:KB * k + KB] = vt[64 * g:64 * g + 32]
                va[g, 48:80, KB * k:KB * k + KB] = vt[64 * g + 32:64 * g + 64]

    def arrive(i):
        remote(kbuf.at[0], kbuf.at[STEPS + i], sib_send.at[i], sib_recv.at[i], sibling).wait_recv()

    def advance(i, following):
        values(i)
        for u in range(UNITS):
            if u + 1 < UNITS:
                score(i, u + 1)
            elif following is not None:
                score(following, 0)
            weigh(u)

    arrive(0)
    score(0, 0)
    advance(0, None)
    handle(1)
    handle(2)
    arrive(1)
    score(1, 0)

    def step(i, carry):
        for k in range(3, STEPS):
            @pl.when(i == k - 2)
            def _():
                handle(k)

        @pl.when(i < STEPS - 1)
        def _():
            arrive(i + 1)

        advance(i, jnp.minimum(i + 1, STEPS - 1))
        return carry

    lax.fori_loop(1, STEPS, step, 0)

    parts = []
    for g in range(3):
        o = [acc[3 * g + t] for t in range(3)]
        o = [v / v[32:33] for v in o]
        parts += [jnp.concatenate([o[0][0:32], o[1][0:32, 0:UW // 2]], axis=1),
                  jnp.concatenate([o[1][48:80, UW // 2:], o[2][48:80]], axis=1)]
    mix_t = jnp.concatenate(parts, axis=0).astype(BF16)
    mix = nt(eye(NQ), mix_t).astype(BF16)
    after_row = res[...] + nn(mix, rw_ref[3])
    n3 = norm(after_row).astype(BF16)
    hidden = nn(n3, up_ref[...])
    hidden = (hidden * 0.5 * (1.0 + lax.erf(hidden * (2.0 ** -0.5)))).astype(BF16)
    out = (after_row + nt(hidden, down_ref[...])).astype(BF16)
    for k in range(NZ):
        os_ref[k] = out[k * RB:(k + 1) * RB]

    side = z // 4
    mine = lax.rem(z, 4)

    def out_copy(d):
        target = {"rows": ((ylo * NX + x) * NZ + lax.rem(z + d, NZ)) * NC + c, "feat": side}
        return remote(os_ref.at[lax.rem(z + d, NZ)], or_ref.at[mine, h], o_send.at[d], o_recv.at[mine, h], target)

    for d in (4, 3, 5, 2, 6, 1, 7):
        out_copy(d).start()

    @pl.when(side == h)
    def _():
        or_ref[mine, h] = os_ref[z]

    @pl.when(side != h)
    def _():
        out_copy(0).start()

    for i in range(4):
        for hs in range(2):
            own = (side == h) & (mine == i) & (h == hs)

            @pl.when(jnp.logical_not(own))
            def _():
                remote(os_ref.at[0], or_ref.at[i, hs], o_send.at[0], o_recv.at[i, hs], partner).wait_recv()

    for hs in range(2):
        blocks = [or_ref[i, hs] for i in range(4)]
        train_out[TR * hs:TR * hs + TR, :] = jnp.concatenate([b[0:TR] for b in blocks], axis=1)
        test_out[TE * hs:TE * hs + TE, :] = jnp.concatenate([b[TR:RB] for b in blocks], axis=1)

    for copy in z_copies:
        copy.wait_send()
    for i in range(STEPS):
        for copy in sends(i):
            copy.wait_send()
        sib_copy(i).wait_send()
    for d in range(1, NZ):
        out_copy(d).wait_send()

    @pl.when(side != h)
    def _():
        out_copy(0).wait_send()


def body(*args):
    args = (*args[:5], args[5].T)
    train, test = args[0], args[1]
    dma = pltpu.SemaphoreType.DMA
    return pl.pallas_call(
        kernel,
        name="layer",
        out_shape=(jax.ShapeDtypeStruct(train.shape, BF16), jax.ShapeDtypeStruct(test.shape, BF16)),
        in_specs=[pl.BlockSpec(memory_space=pl.ANY)] * 6,
        out_specs=(pl.BlockSpec(memory_space=pltpu.VMEM),) * 2,
        scratch_shapes=[pltpu.VMEM(v.shape, BF16) for v in args] + [
            pltpu.VMEM((2, TR, 4 * E), BF16),
            pltpu.VMEM((2, TE, 4 * E), BF16),
            pltpu.VMEM((NQ, E), F32),
            pltpu.VMEM((F, ZB, 128), BF16),
            pltpu.VMEM((NZ, ZB, 128), BF16),
            pltpu.VMEM((2 * STEPS, BLOCK, 128), BF16),
            pltpu.VMEM((UNITS, 2, 256, UW), BF16),
            pltpu.VMEM((2, E, 256), BF16),
            pltpu.VMEM((3, 80, 2 * KB), BF16),
            pltpu.VMEM((3, 2 * KB, UW), F32),
            pltpu.VMEM((UNITS, 80, UW), F32),
            pltpu.VMEM((UNITS, 1, UW), F32),
            pltpu.VMEM((UNITS, 1, UW), F32),
            pltpu.VMEM((NZ, RB, E), BF16),
            pltpu.VMEM((4, 2, RB, E), BF16),
            pltpu.VMEM((NQ, E), F32),
            dma((2,)), dma((2,)), dma((NZ,)), dma((NZ,)),
            dma((STEPS, 4)), dma((STEPS,)), dma((STEPS,)), dma((STEPS,)), dma((STEPS,)),
            dma((NZ,)), dma((4, 2)), dma((6,)),
        ],
        compiler_params=pltpu.CompilerParams(
            collective_id=0, has_side_effects=True, vmem_limit_bytes=60 * 1024 * 1024),
    )(*args)


def solution(mesh):
    return jax.shard_map(
        body,
        mesh=mesh,
        in_specs=(P("rows", "feat"), P("rows", "feat"), P(), P(), P(), P()),
        out_specs=(P("rows", "feat"), P("rows", "feat")),
        check_vma=False,
    )
```

```python
import functools

import jax
import jax.numpy as jnp
from jax import lax
from jax.experimental import pallas as pl
from jax.experimental.pallas import tpu as pltpu
from jax.sharding import PartitionSpec as P

E = 192
HEADS = 6
HD = 32
HID = 768
F = 8
EPS = 1e-05
SCALE = HD ** (-0.5) * 1.4426950408889634
FAR = -1e30
MESH = pl.DeviceIdType.MESH
F32 = jnp.float32
BF16 = jnp.bfloat16

NX, NY, NZ, NC = 4, 4, 8, 2
TR, TE = 32, 16
RB = TR + TE
NQ = NZ * RB
KB = NZ * TR
BLOCK = KB * 3 // 2
HALF = BLOCK // 2
ZB = RB + 2 * TE
STEPS = NX * NY
UW = 256
UNITS = HEADS * NQ // UW

ORDER = [(0, 0), (1, 0), (2, 0), (0, 1), (0, 2), (3, 0), (1, 1), (2, 1),
         (1, 2), (2, 2), (0, 3), (3, 1), (3, 2), (1, 3), (2, 3), (3, 3)]
SLOT = {pos: i for i, pos in enumerate(ORDER)}


def nt(a, b):
    return lax.dot_general(a, b, (((1,), (1,)), ((), ())), preferred_element_type=F32)


def nn(a, b):
    return lax.dot_general(a, b, (((1,), (0,)), ((), ())), preferred_element_type=F32)


def norm(v):
    centred = v - jnp.mean(v, axis=-1, keepdims=True)
    spread = jnp.mean(centred * centred, axis=-1, keepdims=True)
    return centred * lax.rsqrt(spread + EPS)


def eye(n):
    r = lax.broadcasted_iota(jnp.int32, (n, n), 0)
    c = lax.broadcasted_iota(jnp.int32, (n, n), 1)
    return jnp.where(r == c, 1.0, 0.0).astype(BF16)


def head_mask(rows, h):
    lane = lax.broadcasted_iota(jnp.int32, (rows, E), 1)
    return (lane >= h * HD) & (lane < (h + 1) * HD)


def kernel(train_in, test_in, fw_in, rw_in, up_in, down_in,
           train_out, test_out,
           train_ref, test_ref, fw_ref, rw_ref, up_ref, down_ref,
           cell_tr, cell_te, x_ref, zs, zr, kbuf, qp, wv, va, sbuf, acc, m_acc, m_new, os_ref, or_ref, res,
           ex_send, ex_recv, z_send, z_recv, own_send, sib_send, ag_recv, ag_recv2, sib_recv,
           o_send, o_recv, in_sem):
    r = lax.axis_index("rows")
    h = lax.axis_index("feat")
    c = lax.rem(r, NC)
    z = lax.rem(r // NC, NZ)
    x = lax.rem(r // (NC * NZ), NX)
    ylo = r // (NC * NZ * NX)
    y = h * 2 + ylo

    def dev(x_, y_, z_, c_):
        row = ((lax.rem(y_, 2) * NX + x_) * NZ + z_) * NC + c_
        return {"rows": row, "feat": y_ // 2}

    first = jnp.where(c == 0, 1, 0)
    second = 1 - first

    def along(first_step, second_step):
        dx = first * first_step + second * second_step
        dy = second * first_step + first * second_step
        return dev(lax.rem(x + dx + NX, NX), lax.rem(y + dy + NY, NY), z, c)

    a_up, a_down = along(1, 0), along(-1, 0)
    b_up, b_down = along(0, 1), along(0, -1)
    sibling = dev(x, y, z, 1 - c)

    def z_line(d, other):
        return {"rows": ((ylo * NX + x) * NZ + lax.rem(z + d, NZ)) * NC + c,
                "feat": h if not other else 1 - h}

    barrier = pltpu.get_barrier_semaphore()
    for d in range(NZ):
        for other in (False, True):
            if d or other:
                pl.semaphore_signal(barrier, inc=1, device_id=z_line(d, other), device_id_type=MESH)
    for target in (a_up, a_down, b_up, b_down, sibling):
        pl.semaphore_signal(barrier, inc=1, device_id=target, device_id_type=MESH)
    fetch = [pltpu.make_async_copy(a, b, in_sem.at[k]) for k, (a, b) in enumerate((
        (train_in, train_ref), (test_in, test_ref), (fw_in, fw_ref), (rw_in, rw_ref),
        (up_in, up_ref), (down_in, down_ref)))]
    for copy in fetch:
        copy.start()
    fetch[0].wait()
    fetch[1].wait()
    pl.semaphore_wait(barrier, 2 * NZ - 1 + 5)

    def remote(src, dst, send, recv, target):
        return pltpu.make_async_remote_copy(src_ref=src, dst_ref=dst, send_sem=send, recv_sem=recv,
                                            device_id=target, device_id_type=MESH)

    partner = z_line(0, True)
    give_tr = pl.ds(pl.multiple_of((1 - h) * TR, TR), TR)
    give_te = pl.ds(pl.multiple_of((1 - h) * TE, TE), TE)
    ex = [remote(train_ref.at[give_tr], cell_tr.at[h], ex_send.at[0], ex_recv.at[0], partner),
          remote(test_ref.at[give_te], cell_te.at[h], ex_send.at[1], ex_recv.at[1], partner)]
    for copy in ex:
        copy.start()
    keep_tr = pl.ds(pl.multiple_of(h * TR, TR), TR)
    keep_te = pl.ds(pl.multiple_of(h * TE, TE), TE)
    cell_tr[h] = train_ref[keep_tr, :]
    cell_te[h] = test_ref[keep_te, :]
    fetch[2].wait()
    for copy in ex:
        copy.wait()

    for f in range(F):
        lanes = slice((f % 4) * E, (f % 4 + 1) * E)
        for j in range(3):
            if j < 2:
                part = cell_tr[f // 4, 16 * j:16 * j + 16, lanes]
            else:
                part = cell_te[f // 4, :, lanes]
            x_ref[pl.ds(j * 128 + f * 16, 16), :] = part.astype(F32)
    cells = x_ref[...]
    n1 = norm(cells).astype(BF16)
    fq = nn(n1, fw_ref[0]).astype(BF16)
    fk = nn(n1, fw_ref[1]).astype(BF16)
    fv = nn(n1, fw_ref[2]).astype(BF16)
    same = (lax.rem(lax.broadcasted_iota(jnp.int32, (128, 128), 0), 16)
            == lax.rem(lax.broadcasted_iota(jnp.int32, (128, 128), 1), 16))
    zero = jnp.zeros((128, E), BF16)
    rest = []
    for j in range(3):
        rows = slice(128 * j, 128 * j + 128)
        qj, kj, vj = fq[rows], fk[rows], fv[rows]
        mixed = jnp.zeros((128, E), F32)
        for head in range(HEADS):
            mask = head_mask(128, head)
            s = nt(jnp.where(mask, qj, zero), kj) * SCALE
            s = jnp.where(same, s, FAR)
            w = jnp.exp2(s - jnp.max(s, axis=1, keepdims=True))
            total = jnp.sum(w, axis=1, keepdims=True)
            o = nn(w.astype(BF16), vj)
            mixed = jnp.where(mask, o / total, mixed)
        moved = nn(mixed.astype(BF16), fw_ref[3]).astype(BF16).astype(F32)
        after = (cells[rows] + moved).astype(BF16)
        for f in range(F):
            zs[f, 16 * j:16 * j + 16, :] = after[16 * f:16 * f + 16, 0:128]
        rest.append(after[:, 128:E])
    for f in range(F):
        own = slice(16 * f, 16 * f + 16)
        zs[f, RB:RB + TE, :] = jnp.concatenate([rest[0][own], rest[1][own]], axis=1)
        zs[f, RB + TE:ZB, :] = jnp.concatenate([rest[2][own], rest[2][own]], axis=1)

    z_copies = []
    for d in (4, 3, 5, 2, 6, 1, 7):
        copy = remote(zs.at[lax.rem(z + d, NZ)], zr.at[z], z_send.at[d], z_recv.at[d], z_line(d, False))
        copy.start()
        z_copies.append(copy)
    zr[z] = zs[z]
    for copy in z_copies:
        copy.wait_recv()

    for k in range(NZ):
        left = zr[k, 0:RB, :]
        pair = zr[k, RB:RB + TE, :]
        right = jnp.concatenate([pair[:, 0:64], pair[:, 64:128], zr[k, RB + TE:ZB, 0:64]], axis=0)
        res[k * RB:(k + 1) * RB, :] = jnp.concatenate([left, right], axis=1).astype(F32)
    n2 = norm(res[...]).astype(BF16)
    keys = jnp.concatenate([n2[k * RB:k * RB + TR] for k in range(NZ)], axis=0)
    kbuf[0, 0:KB, :] = keys[:, 0:128]
    kbuf[0, KB:BLOCK, :] = jnp.concatenate([keys[0:KB // 2, 128:E], keys[KB // 2:KB, 128:E]], axis=1)

    low, high = pl.ds(0, HALF), pl.ds(HALF, HALF)

    def send_block(slot, which, target, to_slot, rows, recv):
        src = kbuf.at[slot] if rows is None else kbuf.at[slot, rows]
        dst = kbuf.at[to_slot] if rows is None else kbuf.at[to_slot, rows]
        return remote(src, dst, own_send.at[slot, which], recv.at[to_slot], target)

    def sends(i):
        a, b = ORDER[i]
        out = []
        if (a, b) == (0, 0):
            out += [(0, a_up, SLOT[1, 0], None, ag_recv), (1, a_down, SLOT[2, 0], None, ag_recv)]
        if b == 0:
            out += [(2, b_up, SLOT[a, 1], None, ag_recv), (3, b_down, SLOT[a, 2], None, ag_recv)]
        if (a, b) == (1, 0):
            out += [(0, a_up, SLOT[3, 0], low, ag_recv)]
        if (a, b) == (2, 0):
            out += [(0, a_down, SLOT[3, 0], high, ag_recv2)]
        if b == 1:
            out += [(2, b_up, SLOT[a, 3], low, ag_recv)]
        if b == 2:
            out += [(2, b_down, SLOT[a, 3], high, ag_recv2)]
        return [send_block(i, *o) for o in out]

    def sib_copy(i):
        return remote(kbuf.at[i], kbuf.at[STEPS + i], sib_send.at[i], sib_recv.at[i], sibling)

    def handle(i):
        a, b = ORDER[i]
        if i:
            if a == 3 and b == 0 or b == 3:
                remote(kbuf.at[i, low], kbuf.at[i, low], own_send.at[i, 0], ag_recv.at[i], a_up).wait_recv()
                remote(kbuf.at[i, high], kbuf.at[i, high], own_send.at[i, 0], ag_recv2.at[i], a_up).wait_recv()
            else:
                remote(kbuf.at[i], kbuf.at[i], own_send.at[i, 0], ag_recv.at[i], a_up).wait_recv()
        for copy in sends(i):
            copy.start()
        sib_copy(i).start()

    handle(0)

    fetch[3].wait()
    fetch[4].wait()
    fetch[5].wait()
    q2 = nn(n2, rw_ref[0]).astype(BF16)
    wk = rw_ref[1]
    zero = jnp.zeros((E, E), BF16)
    for g in range(HEADS // 2):
        pair = [(nt(jnp.where(head_mask(E, 2 * g + k), wk, zero), q2) * SCALE).astype(BF16) for k in range(2)]
        pair = jnp.concatenate(pair, axis=1)
        for t in range(3):
            part = pair[:, UW * t:UW * t + UW]
            for k in range(2):
                qp[3 * g + t, k, 0:128, :] = part[0:128]
                qp[3 * g + t, k, 128 + 64 * k:192 + 64 * k, :] = part[128:E]
                qp[3 * g + t, k, 192 - 64 * k:256 - 64 * k, :] = jnp.zeros((64, UW), BF16)
    wvt = nt(eye(E), rw_ref[2]).astype(BF16)
    gap = jnp.zeros((E, 64), BF16)
    wv[0] = jnp.concatenate([wvt, gap], axis=1)
    wv[1] = jnp.concatenate([wvt[:, 0:128], gap, wvt[:, 128:E]], axis=1)
    va[...] = jnp.ones_like(va)
    acc[...] = jnp.zeros_like(acc)
    m_acc[...] = jnp.full_like(m_acc, FAR)
    m_new[...] = jnp.full_like(m_new, FAR)

    span = [(0, 48), (0, 80), (32, 80)]

    def half_keys(i, k):
        return jnp.concatenate([
            jnp.concatenate([kbuf[i + STEPS * p, 128 * k:128 * k + 128, :], kbuf[i + STEPS * p, KB:BLOCK, :]], axis=1)
            for p in range(2)], axis=0)

    def score(i, u):
        for k in range(2):
            s = nn(half_keys(i, k), qp[u, k])
            sbuf[u % 3, KB * k:KB * k + KB, :] = s
            m_new[u] = jnp.maximum(m_new[u], jnp.max(s, axis=0, keepdims=True))

    def weigh(u):
        lo, hi = span[u % 3]
        new = m_new[u]
        fade = jnp.exp2(m_acc[u] - new)
        m_acc[u] = new
        w = jnp.exp2(sbuf[u % 3] - new).astype(BF16)
        acc[u, lo:hi, :] = acc[u, lo:hi, :] * fade + nn(va[u // 3, lo:hi, :], w)

    def values(i):
        for k in range(2):
            vt = nt(wv[k], half_keys(i, k)).astype(BF16)
            for g in range(3):
                va[g, 0:32, KB * k:KB * k + KB] = vt[64 * g:64 * g + 32]
                va[g, 48:80, KB * k:KB * k + KB] = vt[64 * g + 32:64 * g + 64]

    def arrive(i):
        remote(kbuf.at[0], kbuf.at[STEPS + i], sib_send.at[i], sib_recv.at[i], sibling).wait_recv()

    def advance(i, following):
        values(i)
        for u in range(UNITS):
            if u + 2 < UNITS:
                score(i, u + 2)
            elif following is not None:
                score(following, u + 2 - UNITS)
            weigh(u)

    arrive(0)
    score(0, 0)
    score(0, 1)
    advance(0, None)
    handle(1)
    handle(2)
    arrive(1)
    score(1, 0)
    score(1, 1)

    def step(i, carry):
        def pick(lo, hi):
            if hi - lo == 1:
                handle(lo + 2)
                return
            mid = (lo + hi) // 2
            pl.when(i < mid)(lambda: pick(lo, mid))
            pl.when(i >= mid)(lambda: pick(mid, hi))

        pl.when(i < STEPS - 2)(lambda: pick(1, STEPS - 2))

        @pl.when(i < STEPS - 1)
        def _():
            arrive(i + 1)

        advance(i, jnp.minimum(i + 1, STEPS - 1))
        return carry

    lax.fori_loop(1, STEPS, step, 0)

    parts = []
    for g in range(3):
        o = [acc[3 * g + t] for t in range(3)]
        o = [v / v[32:33] for v in o]
        parts += [jnp.concatenate([o[0][0:32], o[1][0:32, 0:UW // 2]], axis=1),
                  jnp.concatenate([o[1][48:80, UW // 2:], o[2][48:80]], axis=1)]
    mix_t = jnp.concatenate(parts, axis=0).astype(BF16)
    mix = nt(eye(NQ), mix_t).astype(BF16)
    after_row = res[...] + nn(mix, rw_ref[3])
    n3 = norm(after_row).astype(BF16)
    hidden = nn(n3, up_ref[...])
    hidden = (hidden * 0.5 * (1.0 + lax.erf(hidden * (2.0 ** -0.5)))).astype(BF16)
    out = (after_row + nt(hidden, down_ref[...])).astype(BF16)
    for k in range(NZ):
        os_ref[k] = out[k * RB:(k + 1) * RB]

    side = z // 4
    mine = lax.rem(z, 4)

    def out_copy(d):
        target = {"rows": ((ylo * NX + x) * NZ + lax.rem(z + d, NZ)) * NC + c, "feat": side}
        return remote(os_ref.at[lax.rem(z + d, NZ)], or_ref.at[mine, h], o_send.at[d], o_recv.at[mine, h], target)

    for d in (4, 3, 5, 2, 6, 1, 7):
        out_copy(d).start()

    @pl.when(side == h)
    def _():
        or_ref[mine, h] = os_ref[z]

    @pl.when(side != h)
    def _():
        out_copy(0).start()

    for i in range(4):
        for hs in range(2):
            own = (side == h) & (mine == i) & (h == hs)

            @pl.when(jnp.logical_not(own))
            def _():
                remote(os_ref.at[0], or_ref.at[i, hs], o_send.at[0], o_recv.at[i, hs], partner).wait_recv()

    for hs in range(2):
        blocks = [or_ref[i, hs] for i in range(4)]
        train_out[TR * hs:TR * hs + TR, :] = jnp.concatenate([b[0:TR] for b in blocks], axis=1)
        test_out[TE * hs:TE * hs + TE, :] = jnp.concatenate([b[TR:RB] for b in blocks], axis=1)

    for copy in z_copies:
        copy.wait_send()
    for i in range(STEPS):
        for copy in sends(i):
            copy.wait_send()
        sib_copy(i).wait_send()
    for d in range(1, NZ):
        out_copy(d).wait_send()

    @pl.when(side != h)
    def _():
        out_copy(0).wait_send()


def body(*args):
    args = (*args[:5], args[5].T)
    train, test = args[0], args[1]
    dma = pltpu.SemaphoreType.DMA
    return pl.pallas_call(
        kernel,
        name="layer",
        out_shape=(pltpu.VMEM(train.shape, BF16), pltpu.VMEM(test.shape, BF16)),
        in_specs=[pl.BlockSpec(memory_space=pl.ANY)] * 6,
        out_specs=(pl.BlockSpec(memory_space=pltpu.VMEM),) * 2,
        scratch_shapes=[pltpu.VMEM(v.shape, BF16) for v in args] + [
            pltpu.VMEM((2, TR, 4 * E), BF16),
            pltpu.VMEM((2, TE, 4 * E), BF16),
            pltpu.VMEM((NQ, E), F32),
            pltpu.VMEM((F, ZB, 128), BF16),
            pltpu.VMEM((NZ, ZB, 128), BF16),
            pltpu.VMEM((2 * STEPS, BLOCK, 128), BF16),
            pltpu.VMEM((UNITS, 2, 256, UW), BF16),
            pltpu.VMEM((2, E, 256), BF16),
            pltpu.VMEM((3, 80, 2 * KB), BF16),
            pltpu.VMEM((3, 2 * KB, UW), F32),
            pltpu.VMEM((UNITS, 80, UW), F32),
            pltpu.VMEM((UNITS, 1, UW), F32),
            pltpu.VMEM((UNITS, 1, UW), F32),
            pltpu.VMEM((NZ, RB, E), BF16),
            pltpu.VMEM((4, 2, RB, E), BF16),
            pltpu.VMEM((NQ, E), F32),
            dma((2,)), dma((2,)), dma((NZ,)), dma((NZ,)),
            dma((STEPS, 4)), dma((STEPS,)), dma((STEPS,)), dma((STEPS,)), dma((STEPS,)),
            dma((NZ,)), dma((4, 2)), dma((6,)),
        ],
        compiler_params=pltpu.CompilerParams(
            collective_id=0, has_side_effects=True, vmem_limit_bytes=60 * 1024 * 1024),
    )(*args)


def solution(mesh):
    return jax.shard_map(
        body,
        mesh=mesh,
        in_specs=(P("rows", "feat"), P("rows", "feat"), P(), P(), P(), P()),
        out_specs=(P("rows", "feat"), P("rows", "feat")),
        check_vma=False,
    )
```

```python
import functools

import jax
import jax.numpy as jnp
from jax import lax
from jax.experimental import pallas as pl
from jax.experimental.pallas import tpu as pltpu
from jax.sharding import PartitionSpec as P

E = 192
HEADS = 6
HD = 32
HID = 768
F = 8
EPS = 1e-05
SCALE = HD ** (-0.5) * 1.4426950408889634
FAR = -1e30
MESH = pl.DeviceIdType.MESH
F32 = jnp.float32
BF16 = jnp.bfloat16

NX, NY, NZ, NC = 4, 4, 8, 2
OWN = F // 2
TR, TE = 64, 32
RB = TR + TE
ZB = RB + RB // 2
NS = 4
NQ = NS * RB
KB = NS * TR
BLOCK = KB * 3 // 2
HALF = BLOCK // 2

ORDER = [(0, 0, 0), (0, 1, 0), (0, 0, 1), (0, 0, 2), (0, 1, 1), (0, 1, 2), (0, 0, 3), (0, 1, 3),
         (1, 0, 0), (1, 1, 0), (1, 0, 1), (1, 0, 2), (1, 1, 1), (1, 1, 2), (1, 0, 3), (1, 1, 3)]
SLOT = {pos: i for i, pos in enumerate(ORDER)}
STEPS = len(ORDER)
RELAY = 4
UW = 256
UNITS = HEADS * NQ // UW


def nt(a, b):
    return lax.dot_general(a, b, (((1,), (1,)), ((), ())), preferred_element_type=F32)


def nn(a, b):
    return lax.dot_general(a, b, (((1,), (0,)), ((), ())), preferred_element_type=F32)


def norm(v):
    centred = v - jnp.mean(v, axis=-1, keepdims=True)
    spread = jnp.mean(centred * centred, axis=-1, keepdims=True)
    return centred * lax.rsqrt(spread + EPS)


def eye(n):
    r = lax.broadcasted_iota(jnp.int32, (n, n), 0)
    c = lax.broadcasted_iota(jnp.int32, (n, n), 1)
    return jnp.where(r == c, 1.0, 0.0).astype(BF16)


def pack(ref, at, v):
    ref[at, 0:RB, :] = v[:, 0:128]
    for lo, n in ((0, TR // 2), (TR, TE // 2)):
        ref[at, RB + lo // 2:RB + lo // 2 + n, :] = jnp.concatenate(
            [v[lo:lo + n, 128:E], v[lo + n:lo + 2 * n, 128:E]], axis=1)


def unpack(ref, at):
    right = []
    for lo, n in ((0, TR // 2), (TR, TE // 2)):
        pair = ref[at, RB + lo // 2:RB + lo // 2 + n, :]
        right += [pair[:, 0:64], pair[:, 64:128]]
    return jnp.concatenate([ref[at, 0:RB, :], jnp.concatenate(right, axis=0)], axis=1)


def head_mask(rows, h):
    lane = lax.broadcasted_iota(jnp.int32, (rows, E), 1)
    return (lane >= h * HD) & (lane < (h + 1) * HD)


def kernel(train_in, test_in, fw_in, rw_in, up_in, down_in,
           train_out, test_out,
           train_ref, test_ref, fw_ref, rw_ref, up_ref, down_ref,
           cell_tr, cell_te, x_ref, x2_ref, zs, zr, kbuf, relay, qp, wv, va, sbuf, acc, m_acc, m_new, os_ref, or_ref, res,
           ex_send, ex_recv, z_send, z_recv, own_send, sib_send, ag_recv, ag_recv2, sib_recv,
           o_send, o_recv, rel_send, rel_recv, in_sem):
    r = lax.axis_index("rows")
    h = lax.axis_index("feat")
    c = lax.rem(r, NC)
    z = lax.rem(r // NC, NZ)
    x = lax.rem(r // (NC * NZ), NX)
    ylo = r // (NC * NZ * NX)
    y = h * 2 + ylo

    def dev(x_, y_, z_, c_):
        row = ((lax.rem(y_, 2) * NX + x_) * NZ + z_) * NC + c_
        return {"rows": row, "feat": y_ // 2}

    def dz(d):
        return dev(x, y, lax.rem(z + d + NZ, NZ), c)

    x_up, x_down = dev(lax.rem(x + 1, NX), y, z, c), dev(lax.rem(x + 3, NX), y, z, c)
    y_pair = dev(x, 2 * h + 1 - ylo, z, c)
    sibling = dev(x, y, z, 1 - c)
    partner = dev(x, lax.rem(y + 2, NY), z, c)
    two = jnp.where(lax.rem(z, 2) == 0, 2, -2)
    hop = jnp.where(c == 0, 2, -2)

    barrier = pltpu.get_barrier_semaphore()
    peers = (partner, dz(2), dz(-2), dz(1), dz(-1), x_up, x_down, y_pair, sibling)
    for target in peers:
        pl.semaphore_signal(barrier, inc=1, device_id=target, device_id_type=MESH)
    fetch = [pltpu.make_async_copy(a, b, in_sem.at[k]) for k, (a, b) in enumerate((
        (train_in, train_ref), (test_in, test_ref), (fw_in, fw_ref), (rw_in, rw_ref),
        (up_in, up_ref), (down_in, down_ref)))]
    for copy in fetch:
        copy.start()
    fetch[0].wait()
    fetch[1].wait()
    pl.semaphore_wait(barrier, len(peers))

    def remote(src, dst, send, recv, target):
        return pltpu.make_async_remote_copy(src_ref=src, dst_ref=dst, send_sem=send, recv_sem=recv,
                                            device_id=target, device_id_type=MESH)

    ex = [remote(train_ref, cell_tr, ex_send.at[0], ex_recv.at[0], partner),
          remote(test_ref, cell_te, ex_send.at[1], ex_recv.at[1], partner)]
    for copy in ex:
        copy.start()

    def gather(tr, te, to):
        for f in range(OWN):
            for j in range(RB // 16):
                ref, row = (tr, 16 * j) if j < TR // 16 else (te, 16 * j - TR)
                to[64 * j + 16 * f:64 * j + 16 * f + 16, :] = ref[row:row + 16, f * E:(f + 1) * E].astype(F32)

    gather(train_ref, test_ref, x_ref)
    n1 = norm(x_ref[...]).astype(BF16)
    fetch[2].wait()
    fq = nn(n1, fw_ref[0]).astype(BF16)
    fk = nn(n1, fw_ref[1]).astype(BF16)
    fv = nn(n1, fw_ref[2]).astype(BF16)
    for copy in ex:
        copy.wait_recv()
    gather(cell_tr, cell_te, x2_ref)
    n1 = norm(x2_ref[...]).astype(BF16)
    ok = nn(n1, fw_ref[1]).astype(BF16)
    ov = nn(n1, fw_ref[2]).astype(BF16)
    shape = (HEADS * 64, 128)
    same = (lax.rem(lax.broadcasted_iota(jnp.int32, shape, 0), 16)
            == lax.rem(lax.broadcasted_iota(jnp.int32, shape, 1), 16))
    masks = [head_mask(64, head) for head in range(HEADS)]
    zero = jnp.zeros((64, E), BF16)
    mixes = []
    for j in range(RB // 16):
        rows = slice(64 * j, 64 * j + 64)
        qj = fq[rows]
        kj = jnp.concatenate([fk[rows], ok[rows]], axis=0)
        vj = jnp.concatenate([fv[rows], ov[rows]], axis=0)
        s = nt(jnp.concatenate([jnp.where(m, qj, zero) for m in masks], axis=0), kj) * SCALE
        s = jnp.where(same, s, FAR)
        w = jnp.exp2(s - jnp.max(s, axis=1, keepdims=True))
        o = nn(w.astype(BF16), vj) / jnp.sum(w, axis=1, keepdims=True)
        mixed = o[0:64]
        for head in range(1, HEADS):
            mixed = jnp.where(masks[head], o[64 * head:64 * head + 64], mixed)
        mixes.append(mixed.astype(BF16))
    moved = nn(jnp.concatenate(mixes, axis=0), fw_ref[3]).astype(BF16).astype(F32)
    after = (x_ref[...] + moved).astype(BF16)

    for f in range(OWN):
        pack(zs, f, jnp.concatenate([after[64 * j + 16 * f:64 * j + 16 * f + 16] for j in range(RB // 16)], axis=0))
    z_copies = [remote(zs.at[lax.rem(z + d + NZ, OWN)], zr.at[slot], z_send.at[slot], z_recv.at[slot], dz(d))
                for slot, d in ((3, two), (1, 1), (2, -1))]
    for copy in z_copies:
        copy.start()
    zr[0] = zs[lax.rem(z, OWN)]
    for copy in z_copies:
        copy.wait_recv()

    for k in range(NS):
        res[k * RB:(k + 1) * RB, :] = unpack(zr, k).astype(F32)
    n2 = norm(res[...]).astype(BF16)
    keys = jnp.concatenate([n2[k * RB:k * RB + TR] for k in range(NS)], axis=0)
    kbuf[0, 0:KB, :] = keys[:, 0:128]
    kbuf[0, KB:BLOCK, :] = jnp.concatenate([keys[0:KB // 2, 128:E], keys[KB // 2:KB, 128:E]], axis=1)

    low, high = pl.ds(0, HALF), pl.ds(HALF, HALF)

    def send_block(slot, which, target, to_slot, rows, recv):
        src = kbuf.at[slot] if rows is None else kbuf.at[slot, rows]
        dst = kbuf.at[to_slot] if rows is None else kbuf.at[to_slot, rows]
        return remote(src, dst, own_send.at[slot, which], recv.at[to_slot], target)

    def sends(i):
        t, p, a = ORDER[i]
        out = []
        if (p, a) == (0, 0):
            out += [(2, y_pair, SLOT[t, 1, 0], None, ag_recv)]
        if a == 0:
            out += [(0, x_up, SLOT[t, p, 1], None, ag_recv), (1, x_down, SLOT[t, p, 2], None, ag_recv)]
        if a == 1:
            out += [(0, x_up, SLOT[t, p, 3], low, ag_recv)]
        if a == 2:
            out += [(1, x_down, SLOT[t, p, 3], high, ag_recv2)]
        return [send_block(i, *o) for o in out]

    def sib_copy(i):
        return remote(kbuf.at[i], kbuf.at[STEPS + i], sib_send.at[i], sib_recv.at[i], sibling)

    via = remote(kbuf.at[0], relay, rel_send.at[0], rel_recv.at[0], dz(hop))
    onward = remote(relay, kbuf.at[SLOT[1, 0, 0]], rel_send.at[1], ag_recv.at[SLOT[1, 0, 0]], dz(hop))

    def handle(i):
        t, p, a = ORDER[i]
        if i:
            if a == 3:
                remote(kbuf.at[i, low], kbuf.at[i, low], own_send.at[i, 0], ag_recv.at[i], x_up).wait_recv()
                remote(kbuf.at[i, high], kbuf.at[i, high], own_send.at[i, 0], ag_recv2.at[i], x_up).wait_recv()
            else:
                remote(kbuf.at[i], kbuf.at[i], own_send.at[i, 0], ag_recv.at[i], x_up).wait_recv()
        for copy in sends(i):
            copy.start()
        sib_copy(i).start()

    via.start()
    handle(0)

    fetch[3].wait()
    fetch[4].wait()
    fetch[5].wait()
    q2 = nn(n2, rw_ref[0]).astype(BF16)
    wk = rw_ref[1]
    zero = jnp.zeros((E, E), BF16)
    for g in range(HEADS // 2):
        pair = [(nt(jnp.where(head_mask(E, 2 * g + k), wk, zero), q2) * SCALE).astype(BF16) for k in range(2)]
        pair = jnp.concatenate(pair, axis=1)
        for t in range(3):
            part = pair[:, UW * t:UW * t + UW]
            for k in range(2):
                qp[3 * g + t, k, 0:128, :] = part[0:128]
                qp[3 * g + t, k, 128 + 64 * k:192 + 64 * k, :] = part[128:E]
                qp[3 * g + t, k, 192 - 64 * k:256 - 64 * k, :] = jnp.zeros((64, UW), BF16)
    wvt = nt(eye(E), rw_ref[2]).astype(BF16)
    gap = jnp.zeros((E, 64), BF16)
    wv[0] = jnp.concatenate([wvt, gap], axis=1)
    wv[1] = jnp.concatenate([wvt[:, 0:128], gap, wvt[:, 128:E]], axis=1)
    va[...] = jnp.ones_like(va)
    acc[...] = jnp.zeros_like(acc)
    m_acc[...] = jnp.full_like(m_acc, FAR)
    m_new[...] = jnp.full_like(m_new, FAR)

    span = [(0, 48), (0, 80), (32, 80)]

    def half_keys(i, k):
        return jnp.concatenate([
            jnp.concatenate([kbuf[i + STEPS * p, 128 * k:128 * k + 128, :], kbuf[i + STEPS * p, KB:BLOCK, :]], axis=1)
            for p in range(2)], axis=0)

    def score(i, u):
        for k in range(2):
            s = nn(half_keys(i, k), qp[u, k])
            sbuf[u % 3, KB * k:KB * k + KB, :] = s
            m_new[u] = jnp.maximum(m_new[u], jnp.max(s, axis=0, keepdims=True))

    def weigh(u):
        lo, hi = span[u % 3]
        new = m_new[u]
        fade = jnp.exp2(m_acc[u] - new)
        m_acc[u] = new
        w = jnp.exp2(sbuf[u % 3] - new).astype(BF16)
        acc[u, lo:hi, :] = acc[u, lo:hi, :] * fade + nn(va[u // 3, lo:hi, :], w)

    def values(i):
        for k in range(2):
            vt = nt(wv[k], half_keys(i, k)).astype(BF16)
            for g in range(3):
                va[g, 0:32, KB * k:KB * k + KB] = vt[64 * g:64 * g + 32]
                va[g, 48:80, KB * k:KB * k + KB] = vt[64 * g + 32:64 * g + 64]

    def arrive(i):
        remote(kbuf.at[0], kbuf.at[STEPS + i], sib_send.at[i], sib_recv.at[i], sibling).wait_recv()

    def advance(i, following):
        values(i)
        for u in range(UNITS):
            if u + 2 < UNITS:
                score(i, u + 2)
            elif following is not None:
                score(following, u + 2 - UNITS)
            weigh(u)

    arrive(0)
    score(0, 0)
    score(0, 1)
    advance(0, None)
    handle(1)
    handle(2)
    arrive(1)
    score(1, 0)
    score(1, 1)

    def step(i, carry):
        def pick(lo, hi):
            if hi - lo == 1:
                if lo + 2 == RELAY:
                    via.wait_recv()
                    onward.start()
                handle(lo + 2)
                return
            mid = (lo + hi) // 2
            pl.when(i < mid)(lambda: pick(lo, mid))
            pl.when(i >= mid)(lambda: pick(mid, hi))

        pl.when(i < STEPS - 2)(lambda: pick(1, STEPS - 2))

        @pl.when(i < STEPS - 1)
        def _():
            arrive(i + 1)

        advance(i, jnp.minimum(i + 1, STEPS - 1))
        return carry

    lax.fori_loop(1, STEPS, step, 0)

    parts = []
    for g in range(3):
        o = [acc[3 * g + t] for t in range(3)]
        o = [v / v[32:33] for v in o]
        parts += [jnp.concatenate([o[0][0:32], o[1][0:32, 0:UW // 2]], axis=1),
                  jnp.concatenate([o[1][48:80, UW // 2:], o[2][48:80]], axis=1)]
    mix_t = jnp.concatenate(parts, axis=0).astype(BF16)
    mix = nt(eye(NQ), mix_t).astype(BF16)
    after_row = res[...] + nn(mix, rw_ref[3])
    n3 = norm(after_row).astype(BF16)
    hidden = nn(n3, up_ref[...])
    hidden = (hidden * 0.5 * (1.0 + lax.erf(hidden * (2.0 ** -0.5)))).astype(BF16)
    out = (after_row + nt(hidden, down_ref[...])).astype(BF16)
    for k in range(NS):
        pack(os_ref, k, out[k * RB:(k + 1) * RB])

    mine = lax.rem(z, OWN)
    o_copies = [remote(os_ref.at[slot], or_ref.at[mine], o_send.at[slot], o_recv.at[mine], dz(d))
                for slot, d in ((3, -two), (1, -1), (2, 1))]
    for copy in o_copies:
        copy.start()
    or_ref[mine] = os_ref[0]
    for d in (1, -1, 2):
        f = lax.rem(z + d + NZ, OWN)
        remote(os_ref.at[0], or_ref.at[f], o_send.at[0], o_recv.at[f], sibling).wait_recv()
    blocks = [unpack(or_ref, f) for f in range(OWN)]
    train_out[...] = jnp.concatenate([v[0:TR] for v in blocks], axis=1)
    test_out[...] = jnp.concatenate([v[TR:RB] for v in blocks], axis=1)

    for copy in ex + z_copies + o_copies + [via, onward]:
        copy.wait_send()
    for i in range(STEPS):
        for copy in sends(i):
            copy.wait_send()
        sib_copy(i).wait_send()


def body(*args):
    args = (*args[:5], args[5].T)
    train, test = args[0], args[1]
    dma = pltpu.SemaphoreType.DMA
    return pl.pallas_call(
        kernel,
        name="layer",
        out_shape=(pltpu.VMEM(train.shape, BF16), pltpu.VMEM(test.shape, BF16)),
        in_specs=[pl.BlockSpec(memory_space=pl.ANY)] * 6,
        out_specs=(pl.BlockSpec(memory_space=pltpu.VMEM),) * 2,
        scratch_shapes=[pltpu.VMEM(v.shape, BF16) for v in args] + [
            pltpu.VMEM((TR, OWN * E), BF16),
            pltpu.VMEM((TE, OWN * E), BF16),
            pltpu.VMEM((OWN * RB, E), F32),
            pltpu.VMEM((OWN * RB, E), F32),
            pltpu.VMEM((OWN, ZB, 128), BF16),
            pltpu.VMEM((NS, ZB, 128), BF16),
            pltpu.VMEM((2 * STEPS, BLOCK, 128), BF16),
            pltpu.VMEM((BLOCK, 128), BF16),
            pltpu.VMEM((UNITS, 2, 256, UW), BF16),
            pltpu.VMEM((2, E, 256), BF16),
            pltpu.VMEM((3, 80, 2 * KB), BF16),
            pltpu.VMEM((3, 2 * KB, UW), F32),
            pltpu.VMEM((UNITS, 80, UW), F32),
            pltpu.VMEM((UNITS, 1, UW), F32),
            pltpu.VMEM((UNITS, 1, UW), F32),
            pltpu.VMEM((NS, ZB, 128), BF16),
            pltpu.VMEM((OWN, ZB, 128), BF16),
            pltpu.VMEM((NQ, E), F32),
            dma((2,)), dma((2,)), dma((NS,)), dma((NS,)),
            dma((STEPS, 4)), dma((STEPS,)), dma((STEPS,)), dma((STEPS,)), dma((STEPS,)),
            dma((NS,)), dma((OWN,)), dma((2,)), dma((1,)), dma((6,)),
        ],
        compiler_params=pltpu.CompilerParams(
            collective_id=0, has_side_effects=True, vmem_limit_bytes=60 * 1024 * 1024),
    )(*args)


def solution(mesh):
    return jax.shard_map(
        body,
        mesh=mesh,
        in_specs=(P("rows", "feat"), P("rows", "feat"), P(), P(), P(), P()),
        out_specs=(P("rows", "feat"), P("rows", "feat")),
        check_vma=False,
    )
```

```python
import functools

import jax
import jax.numpy as jnp
from jax import lax
from jax.experimental import pallas as pl
from jax.experimental.pallas import tpu as pltpu
from jax.sharding import PartitionSpec as P

E = 192
HEADS = 6
HD = 32
HID = 768
F = 8
EPS = 1e-05
SCALE = HD ** (-0.5) * 1.4426950408889634
FAR = -1e30
MESH = pl.DeviceIdType.MESH
F32 = jnp.float32
BF16 = jnp.bfloat16

NX, NY, NZ, NC = 4, 4, 8, 2
OWN = F // 2
TR, TE = 64, 32
RB = TR + TE
ZB = RB + RB // 2
PR = 32
PB = PR + PR // 2
PIECES = RB // PR
NS = 4
NQ = NS * RB
KB = NS * TR
BLOCK = KB * 3 // 2
HALF = BLOCK // 2

ORDER = [(0, 0, 0), (0, 1, 0), (0, 0, 1), (0, 0, 2), (0, 1, 1), (0, 1, 2), (1, 0, 0), (0, 0, 3),
         (0, 1, 3), (1, 1, 0), (1, 0, 1), (1, 0, 2), (1, 1, 1), (1, 1, 2), (1, 0, 3), (1, 1, 3)]
SLOT = {pos: i for i, pos in enumerate(ORDER)}
STEPS = len(ORDER)
RELAY = 3
UW = 256
UNITS = HEADS * NQ // UW


def nt(a, b):
    return lax.dot_general(a, b, (((1,), (1,)), ((), ())), preferred_element_type=F32)


def nn(a, b):
    return lax.dot_general(a, b, (((1,), (0,)), ((), ())), preferred_element_type=F32)


def norm(v):
    centred = v - jnp.mean(v, axis=-1, keepdims=True)
    spread = jnp.mean(centred * centred, axis=-1, keepdims=True)
    return centred * lax.rsqrt(spread + EPS)


def eye(n):
    r = lax.broadcasted_iota(jnp.int32, (n, n), 0)
    c = lax.broadcasted_iota(jnp.int32, (n, n), 1)
    return jnp.where(r == c, 1.0, 0.0).astype(BF16)


def pack_piece(ref, at, q, v):
    ref[at, q * PB:q * PB + PR, :] = v[:, 0:128]
    ref[at, q * PB + PR:(q + 1) * PB, :] = jnp.concatenate([v[0:PR // 2, 128:E], v[PR // 2:PR, 128:E]], axis=1)


def unpack(ref, at):
    out = []
    for q in range(RB // PR):
        pair = ref[at, q * PB + PR:(q + 1) * PB, :]
        right = jnp.concatenate([pair[:, 0:64], pair[:, 64:128]], axis=0)
        out.append(jnp.concatenate([ref[at, q * PB:q * PB + PR, :], right], axis=1))
    return jnp.concatenate(out, axis=0)


def head_mask(rows, h):
    lane = lax.broadcasted_iota(jnp.int32, (rows, E), 1)
    return (lane >= h * HD) & (lane < (h + 1) * HD)


def kernel(train_in, test_in, fw_in, rw_in, up_in, down_in,
           train_out, test_out,
           train_ref, test_ref, fw_ref, rw_ref, up_ref, down_ref,
           cell_tr, cell_te, x_ref, zs, zr, kbuf, relay, qp, wv, va, sbuf, acc, m_acc, m_new, os_ref, or_ref, res,
           ex_send, ex_recv, z_send, z_recv, own_send, sib_send, ag_recv, ag_recv2, sib_recv,
           o_send, o_recv, rel_send, rel_recv, in_sem):
    r = lax.axis_index("rows")
    h = lax.axis_index("feat")
    c = lax.rem(r, NC)
    z = lax.rem(r // NC, NZ)
    x = lax.rem(r // (NC * NZ), NX)
    ylo = r // (NC * NZ * NX)
    y = h * 2 + ylo

    def dev(x_, y_, z_, c_):
        row = ((lax.rem(y_, 2) * NX + x_) * NZ + z_) * NC + c_
        return {"rows": row, "feat": y_ // 2}

    def dz(d):
        return dev(x, y, lax.rem(z + d + NZ, NZ), c)

    x_up, x_down = dev(lax.rem(x + 1, NX), y, z, c), dev(lax.rem(x + 3, NX), y, z, c)
    y_other = 2 * h + 1 - ylo
    y_pair = dev(x, y_other, z, c)
    d_up, d_down = dev(lax.rem(x + 1, NX), y_other, z, c), dev(lax.rem(x + 3, NX), y_other, z, c)
    sibling = dev(x, y, z, 1 - c)
    partner = dev(x, lax.rem(y + 2, NY), z, c)
    two = jnp.where(lax.rem(z, 2) == 0, 2, -2)
    hop = jnp.where(c == 0, 2, -2)

    barrier = pltpu.get_barrier_semaphore()
    peers = (partner, dz(2), dz(-2), d_up, d_down, dz(1), dz(-1), x_up, x_down, y_pair, sibling)
    for target in peers:
        pl.semaphore_signal(barrier, inc=1, device_id=target, device_id_type=MESH)
    fetch = [pltpu.make_async_copy(a, b, in_sem.at[k]) for k, (a, b) in enumerate((
        (train_in, train_ref), (test_in, test_ref), (fw_in, fw_ref), (rw_in, rw_ref),
        (up_in, up_ref), (down_in, down_ref)))]
    for copy in fetch:
        copy.start()
    fetch[0].wait()
    fetch[1].wait()
    pl.semaphore_wait(barrier, len(peers))

    def remote(src, dst, send, recv, target):
        return pltpu.make_async_remote_copy(src_ref=src, dst_ref=dst, send_sem=send, recv_sem=recv,
                                            device_id=target, device_id_type=MESH)

    spots = [(train_ref, cell_tr, 0), (train_ref, cell_tr, PR), (test_ref, cell_te, 0)]
    ex = [remote(src.at[pl.ds(at, PR)], dst.at[pl.ds(at, PR)], ex_send.at[q], ex_recv.at[q], partner)
          for q, (src, dst, at) in enumerate(spots)]
    for copy in ex:
        copy.start()

    def gather(ref, at):
        return jnp.concatenate([ref[at + 16 * j:at + 16 * j + 16, f * E:(f + 1) * E]
                                for j in range(PR // 16) for f in range(OWN)], axis=0).astype(F32)

    shape = (HEADS * 64, 128)
    same = (lax.rem(lax.broadcasted_iota(jnp.int32, shape, 0), 16)
            == lax.rem(lax.broadcasted_iota(jnp.int32, shape, 1), 16))
    masks = [head_mask(64, head) for head in range(HEADS)]
    zero = jnp.zeros((64, E), BF16)
    for q, (src, dst, at) in enumerate(spots):
        x_ref[q] = gather(src, at)
    fetch[2].wait()
    own = norm(x_ref[...].reshape(OWN * RB, E)).astype(BF16)
    fq = nn(own, fw_ref[0]).astype(BF16)
    fk = nn(own, fw_ref[1]).astype(BF16)
    fv = nn(own, fw_ref[2]).astype(BF16)
    z_copies = []
    for q, (src, dst, at) in enumerate(spots):
        ex[q].wait_recv()
        other = norm(gather(dst, at)).astype(BF16)
        ok = nn(other, fw_ref[1]).astype(BF16)
        ov = nn(other, fw_ref[2]).astype(BF16)
        mixes = []
        for j in range(PR // 16):
            here, there = slice(64 * j, 64 * j + 64), slice(128 * q + 64 * j, 128 * q + 64 * j + 64)
            qj = fq[there]
            kj = jnp.concatenate([fk[there], ok[here]], axis=0)
            vj = jnp.concatenate([fv[there], ov[here]], axis=0)
            s = nt(jnp.concatenate([jnp.where(m, qj, zero) for m in masks], axis=0), kj) * SCALE
            s = jnp.where(same, s, FAR)
            w = jnp.exp2(s - jnp.max(s, axis=1, keepdims=True))
            o = nn(w.astype(BF16), vj) / jnp.sum(w, axis=1, keepdims=True)
            mixed = o[0:64]
            for head in range(1, HEADS):
                mixed = jnp.where(masks[head], o[64 * head:64 * head + 64], mixed)
            mixes.append(mixed.astype(BF16))
        moved = nn(jnp.concatenate(mixes, axis=0), fw_ref[3]).astype(BF16).astype(F32)
        after = (x_ref[q] + moved).astype(BF16)
        for f in range(OWN):
            part = jnp.concatenate([after[64 * j + 16 * f:64 * j + 16 * f + 16] for j in range(PR // 16)], axis=0)
            pack_piece(zs, f, q, part)
        rows = pl.ds(q * PB, PB)
        for slot, d in ((3, two), (1, 1), (2, -1)):
            copy = remote(zs.at[lax.rem(z + d + NZ, OWN), rows], zr.at[slot, rows],
                          z_send.at[slot, q], z_recv.at[slot, q], dz(d))
            copy.start()
            z_copies.append(copy)
    zr[0] = zs[lax.rem(z, OWN)]
    for copy in z_copies:
        copy.wait_recv()

    for k in range(NS):
        res[k * RB:(k + 1) * RB, :] = unpack(zr, k).astype(F32)
    n2 = norm(res[...]).astype(BF16)
    keys = jnp.concatenate([n2[k * RB:k * RB + TR] for k in range(NS)], axis=0)
    kbuf[0, 0:KB, :] = keys[:, 0:128]
    kbuf[0, KB:BLOCK, :] = jnp.concatenate([keys[0:KB // 2, 128:E], keys[KB // 2:KB, 128:E]], axis=1)

    low, high = pl.ds(0, HALF), pl.ds(HALF, HALF)

    def send_block(slot, which, target, to_slot, rows, recv):
        src = kbuf.at[slot] if rows is None else kbuf.at[slot, rows]
        dst = kbuf.at[to_slot] if rows is None else kbuf.at[to_slot, rows]
        return remote(src, dst, own_send.at[slot, which], recv.at[to_slot], target)

    def sends(i):
        t, p, a = ORDER[i]
        out = []
        if (p, a) == (0, 0):
            out += [(0, x_up, SLOT[t, 0, 1], None, ag_recv), (1, x_down, SLOT[t, 0, 2], None, ag_recv),
                    (2, y_pair, SLOT[t, 1, 0], None, ag_recv),
                    (3, d_up, SLOT[t, 1, 1], None, ag_recv), (4, d_down, SLOT[t, 1, 2], None, ag_recv)]
        if a == 1:
            out += [(0, x_up, SLOT[t, p, 3], low, ag_recv)]
        if a == 2:
            out += [(1, x_down, SLOT[t, p, 3], high, ag_recv2)]
        return [send_block(i, *o) for o in out]

    def sib_copy(i):
        return remote(kbuf.at[i], kbuf.at[STEPS + i], sib_send.at[i], sib_recv.at[i], sibling)

    via = remote(kbuf.at[0], relay, rel_send.at[0], rel_recv.at[0], dz(hop))
    onward = remote(relay, kbuf.at[SLOT[1, 0, 0]], rel_send.at[1], ag_recv.at[SLOT[1, 0, 0]], dz(hop))

    def handle(i):
        t, p, a = ORDER[i]
        if i:
            if a == 3:
                remote(kbuf.at[i, low], kbuf.at[i, low], own_send.at[i, 0], ag_recv.at[i], x_up).wait_recv()
                remote(kbuf.at[i, high], kbuf.at[i, high], own_send.at[i, 0], ag_recv2.at[i], x_up).wait_recv()
            else:
                remote(kbuf.at[i], kbuf.at[i], own_send.at[i, 0], ag_recv.at[i], x_up).wait_recv()
        for copy in sends(i):
            copy.start()
        sib_copy(i).start()

    via.start()
    handle(0)

    fetch[3].wait()
    fetch[4].wait()
    fetch[5].wait()
    q2 = nn(n2, rw_ref[0]).astype(BF16)
    wk = rw_ref[1]
    zero = jnp.zeros((E, E), BF16)
    for g in range(HEADS // 2):
        pair = [(nt(jnp.where(head_mask(E, 2 * g + k), wk, zero), q2) * SCALE).astype(BF16) for k in range(2)]
        pair = jnp.concatenate(pair, axis=1)
        for t in range(3):
            part = pair[:, UW * t:UW * t + UW]
            for k in range(2):
                qp[3 * g + t, k, 0:128, :] = part[0:128]
                qp[3 * g + t, k, 128 + 64 * k:192 + 64 * k, :] = part[128:E]
                qp[3 * g + t, k, 192 - 64 * k:256 - 64 * k, :] = jnp.zeros((64, UW), BF16)
    wvt = nt(eye(E), rw_ref[2]).astype(BF16)
    gap = jnp.zeros((E, 64), BF16)
    wv[0] = jnp.concatenate([wvt, gap], axis=1)
    wv[1] = jnp.concatenate([wvt[:, 0:128], gap, wvt[:, 128:E]], axis=1)
    va[...] = jnp.ones_like(va)
    acc[...] = jnp.zeros_like(acc)
    m_acc[...] = jnp.full_like(m_acc, FAR)
    m_new[...] = jnp.full_like(m_new, FAR)

    span = [(0, 48), (0, 80), (32, 80)]

    def half_keys(i, k):
        return jnp.concatenate([
            jnp.concatenate([kbuf[i + STEPS * p, 128 * k:128 * k + 128, :], kbuf[i + STEPS * p, KB:BLOCK, :]], axis=1)
            for p in range(2)], axis=0)

    def score(i, u):
        for k in range(2):
            s = nn(half_keys(i, k), qp[u, k])
            sbuf[u, KB * k:KB * k + KB, :] = s
            m_new[u] = jnp.maximum(m_new[u], jnp.max(s, axis=0, keepdims=True))

    def weigh(u):
        lo, hi = span[u % 3]
        new = m_new[u]
        fade = jnp.exp2(m_acc[u] - new)
        m_acc[u] = new
        w = jnp.exp2(sbuf[u] - new).astype(BF16)
        acc[u, lo:hi, :] = acc[u, lo:hi, :] * fade + nn(va[u // 3, lo:hi, :], w)

    def values(i):
        for k in range(2):
            vt = nt(wv[k], half_keys(i, k)).astype(BF16)
            for g in range(3):
                va[g, 0:32, KB * k:KB * k + KB] = vt[64 * g:64 * g + 32]
                va[g, 48:80, KB * k:KB * k + KB] = vt[64 * g + 32:64 * g + 64]

    def arrive(i):
        remote(kbuf.at[0], kbuf.at[STEPS + i], sib_send.at[i], sib_recv.at[i], sibling).wait_recv()

    def advance(i, following):
        values(i)
        for u in range(UNITS):
            if u + 3 < UNITS:
                score(i, u + 3)
            elif following is not None:
                score(following, u + 3 - UNITS)
            weigh(u)

    arrive(0)
    score(0, 0)
    score(0, 1)
    score(0, 2)
    advance(0, None)
    handle(1)
    handle(2)
    arrive(1)
    score(1, 0)
    score(1, 1)
    score(1, 2)

    def step(i, carry):
        def pick(lo, hi):
            if hi - lo == 1:
                if lo + 2 == RELAY:
                    via.wait_recv()
                    onward.start()
                handle(lo + 2)
                return
            mid = (lo + hi) // 2
            pl.when(i < mid)(lambda: pick(lo, mid))
            pl.when(i >= mid)(lambda: pick(mid, hi))

        pl.when(i < STEPS - 2)(lambda: pick(1, STEPS - 2))

        @pl.when(i < STEPS - 1)
        def _():
            arrive(i + 1)

        advance(i, jnp.minimum(i + 1, STEPS - 1))
        return carry

    lax.fori_loop(1, STEPS, step, 0)

    parts = []
    for g in range(3):
        o = [acc[3 * g + t] for t in range(3)]
        o = [v / v[32:33] for v in o]
        parts += [jnp.concatenate([o[0][0:32], o[1][0:32, 0:UW // 2]], axis=1),
                  jnp.concatenate([o[1][48:80, UW // 2:], o[2][48:80]], axis=1)]
    mix_t = jnp.concatenate(parts, axis=0).astype(BF16)
    mix = nt(eye(NQ), mix_t).astype(BF16)
    mine = lax.rem(z, OWN)
    o_copies = []
    for slot, d in ((3, -two), (1, -1), (2, 1), (0, 0)):
        rows = slice(slot * RB, slot * RB + RB)
        after_row = res[rows, :] + nn(mix[rows], rw_ref[3])
        n3 = norm(after_row).astype(BF16)
        hidden = nn(n3, up_ref[...])
        hidden = (hidden * 0.5 * (1.0 + lax.erf(hidden * (2.0 ** -0.5)))).astype(BF16)
        out = (after_row + nt(hidden, down_ref[...])).astype(BF16)
        for q in range(PIECES):
            pack_piece(os_ref, slot, q, out[q * PR:(q + 1) * PR])
        if slot:
            copy = remote(os_ref.at[slot], or_ref.at[mine], o_send.at[slot], o_recv.at[mine], dz(d))
            copy.start()
            o_copies.append(copy)
    or_ref[mine] = os_ref[0]
    for d in (1, -1, 2):
        f = lax.rem(z + d + NZ, OWN)
        remote(os_ref.at[0], or_ref.at[f], o_send.at[0], o_recv.at[f], sibling).wait_recv()
    blocks = [unpack(or_ref, f) for f in range(OWN)]
    train_out[...] = jnp.concatenate([v[0:TR] for v in blocks], axis=1)
    test_out[...] = jnp.concatenate([v[TR:RB] for v in blocks], axis=1)

    for copy in ex + z_copies + o_copies + [via, onward]:
        copy.wait_send()
    for i in range(STEPS):
        for copy in sends(i):
            copy.wait_send()
        sib_copy(i).wait_send()


def body(*args):
    args = (*args[:5], args[5].T)
    train, test = args[0], args[1]
    dma = pltpu.SemaphoreType.DMA
    return pl.pallas_call(
        kernel,
        name="layer",
        out_shape=(pltpu.VMEM(train.shape, BF16), pltpu.VMEM(test.shape, BF16)),
        in_specs=[pl.BlockSpec(memory_space=pl.ANY)] * 6,
        out_specs=(pl.BlockSpec(memory_space=pltpu.VMEM),) * 2,
        scratch_shapes=[pltpu.VMEM(v.shape, BF16) for v in args] + [
            pltpu.VMEM((TR, OWN * E), BF16),
            pltpu.VMEM((TE, OWN * E), BF16),
            pltpu.VMEM((PIECES, OWN * PR, E), F32),
            pltpu.VMEM((OWN, ZB, 128), BF16),
            pltpu.VMEM((NS, ZB, 128), BF16),
            pltpu.VMEM((2 * STEPS, BLOCK, 128), BF16),
            pltpu.VMEM((BLOCK, 128), BF16),
            pltpu.VMEM((UNITS, 2, 256, UW), BF16),
            pltpu.VMEM((2, E, 256), BF16),
            pltpu.VMEM((3, 80, 2 * KB), BF16),
            pltpu.VMEM((UNITS, 2 * KB, UW), F32),
            pltpu.VMEM((UNITS, 80, UW), F32),
            pltpu.VMEM((UNITS, 1, UW), F32),
            pltpu.VMEM((UNITS, 1, UW), F32),
            pltpu.VMEM((NS, ZB, 128), BF16),
            pltpu.VMEM((OWN, ZB, 128), BF16),
            pltpu.VMEM((NQ, E), F32),
            dma((PIECES,)), dma((PIECES,)), dma((NS, PIECES)), dma((NS, PIECES)),
            dma((STEPS, 5)), dma((STEPS,)), dma((STEPS,)), dma((STEPS,)), dma((STEPS,)),
            dma((NS,)), dma((OWN,)), dma((2,)), dma((1,)), dma((6,)),
        ],
        compiler_params=pltpu.CompilerParams(
            collective_id=0, has_side_effects=True, vmem_limit_bytes=60 * 1024 * 1024),
    )(*args)


def solution(mesh):
    return jax.shard_map(
        body,
        mesh=mesh,
        in_specs=(P("rows", "feat"), P("rows", "feat"), P(), P(), P(), P()),
        out_specs=(P("rows", "feat"), P("rows", "feat")),
        check_vma=False,
    )
```

```python
import functools

import jax
import jax.numpy as jnp
from jax import lax
from jax.experimental import pallas as pl
from jax.experimental.pallas import tpu as pltpu
from jax.sharding import PartitionSpec as P

E = 192
HEADS = 6
HD = 32
HID = 768
F = 8
EPS = 1e-05
SCALE = HD ** (-0.5) * 1.4426950408889634
FAR = -1e30
MESH = pl.DeviceIdType.MESH
F32 = jnp.float32
BF16 = jnp.bfloat16

NX, NY, NZ, NC = 4, 4, 8, 2
OWN = F // 2
TR, TE = 64, 32
RB = TR + TE
ZB = RB + RB // 2
NS = 4
NQ = NS * RB
KB = NS * TR
BLOCK = KB * 3 // 2
HALF = BLOCK // 2

ORDER = [(0, 0, 0), (0, 1, 0), (0, 0, 1), (0, 0, 2), (0, 1, 1), (0, 1, 2), (1, 0, 0), (0, 0, 3),
         (0, 1, 3), (1, 1, 0), (1, 0, 1), (1, 0, 2), (1, 1, 1), (1, 1, 2), (1, 0, 3), (1, 1, 3)]
SLOT = {pos: i for i, pos in enumerate(ORDER)}
STEPS = len(ORDER)
UW = 256
UNITS = HEADS * NQ // UW


def nt(a, b):
    return lax.dot_general(a, b, (((1,), (1,)), ((), ())), preferred_element_type=F32)


def nn(a, b):
    return lax.dot_general(a, b, (((1,), (0,)), ((), ())), preferred_element_type=F32)


def norm(v):
    centred = v - jnp.mean(v, axis=-1, keepdims=True)
    spread = jnp.mean(centred * centred, axis=-1, keepdims=True)
    return centred * lax.rsqrt(spread + EPS)


def eye(n):
    r = lax.broadcasted_iota(jnp.int32, (n, n), 0)
    c = lax.broadcasted_iota(jnp.int32, (n, n), 1)
    return jnp.where(r == c, 1.0, 0.0).astype(BF16)


def pack(ref, at, v):
    ref[at, 0:RB, :] = v[:, 0:128]
    for lo, n in ((0, TR // 2), (TR, TE // 2)):
        ref[at, RB + lo // 2:RB + lo // 2 + n, :] = jnp.concatenate(
            [v[lo:lo + n, 128:E], v[lo + n:lo + 2 * n, 128:E]], axis=1)


def unpack(ref, at):
    right = []
    for lo, n in ((0, TR // 2), (TR, TE // 2)):
        pair = ref[at, RB + lo // 2:RB + lo // 2 + n, :]
        right += [pair[:, 0:64], pair[:, 64:128]]
    return jnp.concatenate([ref[at, 0:RB, :], jnp.concatenate(right, axis=0)], axis=1)


def head_mask(rows, h):
    lane = lax.broadcasted_iota(jnp.int32, (rows, E), 1)
    return (lane >= h * HD) & (lane < (h + 1) * HD)


def kernel(train_in, test_in, fw_in, rw_in, up_in, down_in,
           train_out, test_out,
           train_ref, test_ref, fw_ref, rw_ref, up_ref, down_ref,
           cell_tr, cell_te, x_ref, x2_ref, zs, zr, kbuf, qp, wv, va, sbuf, acc, m_acc, m_new, os_ref, or_ref, res,
           ex_send, ex_recv, z_send, z_recv, own_send, sib_send, ag_recv, ag_recv2, sib_recv,
           o_send, o_recv, far_send, in_sem):
    r = lax.axis_index("rows")
    h = lax.axis_index("feat")
    c = lax.rem(r, NC)
    z = lax.rem(r // NC, NZ)
    x = lax.rem(r // (NC * NZ), NX)
    ylo = r // (NC * NZ * NX)
    y = h * 2 + ylo

    def dev(x_, y_, z_, c_):
        row = ((lax.rem(y_, 2) * NX + x_) * NZ + z_) * NC + c_
        return {"rows": row, "feat": y_ // 2}

    def dz(d):
        return dev(x, y, lax.rem(z + d + NZ, NZ), c)

    x_up, x_down = dev(lax.rem(x + 1, NX), y, z, c), dev(lax.rem(x + 3, NX), y, z, c)
    y_pair = dev(x, 2 * h + 1 - ylo, z, c)
    sibling = dev(x, y, z, 1 - c)
    partner = dev(x, lax.rem(y + 2, NY), z, c)
    two = jnp.where(lax.rem(z, 2) == 0, 2, -2)

    barrier = pltpu.get_barrier_semaphore()
    peers = (partner, dz(2), dz(-2), dz(1), dz(-1), x_up, x_down, y_pair, sibling)
    for target in peers:
        pl.semaphore_signal(barrier, inc=1, device_id=target, device_id_type=MESH)
    fetch = [pltpu.make_async_copy(a, b, in_sem.at[k]) for k, (a, b) in enumerate((
        (train_in, train_ref), (test_in, test_ref), (fw_in, fw_ref), (rw_in, rw_ref),
        (up_in, up_ref), (down_in, down_ref)))]
    for copy in fetch:
        copy.start()
    fetch[0].wait()
    fetch[1].wait()
    pl.semaphore_wait(barrier, len(peers))

    def remote(src, dst, send, recv, target):
        return pltpu.make_async_remote_copy(src_ref=src, dst_ref=dst, send_sem=send, recv_sem=recv,
                                            device_id=target, device_id_type=MESH)

    ex = [remote(train_ref, cell_tr, ex_send.at[0], ex_recv.at[0], partner),
          remote(test_ref, cell_te, ex_send.at[1], ex_recv.at[1], partner)]
    for copy in ex:
        copy.start()

    def gather(tr, te, to):
        for f in range(OWN):
            for j in range(RB // 16):
                ref, row = (tr, 16 * j) if j < TR // 16 else (te, 16 * j - TR)
                to[64 * j + 16 * f:64 * j + 16 * f + 16, :] = ref[row:row + 16, f * E:(f + 1) * E].astype(F32)

    gather(train_ref, test_ref, x_ref)
    n1 = norm(x_ref[...]).astype(BF16)
    fetch[2].wait()
    fq = nn(n1, fw_ref[0]).astype(BF16)
    fk = nn(n1, fw_ref[1]).astype(BF16)
    fv = nn(n1, fw_ref[2]).astype(BF16)
    for copy in ex:
        copy.wait_recv()
    gather(cell_tr, cell_te, x2_ref)
    n1 = norm(x2_ref[...]).astype(BF16)
    ok = nn(n1, fw_ref[1]).astype(BF16)
    ov = nn(n1, fw_ref[2]).astype(BF16)
    shape = (HEADS * 64, 128)
    same = (lax.rem(lax.broadcasted_iota(jnp.int32, shape, 0), 16)
            == lax.rem(lax.broadcasted_iota(jnp.int32, shape, 1), 16))
    masks = [head_mask(64, head) for head in range(HEADS)]
    zero = jnp.zeros((64, E), BF16)
    mixes = []
    for j in range(RB // 16):
        rows = slice(64 * j, 64 * j + 64)
        qj = fq[rows]
        kj = jnp.concatenate([fk[rows], ok[rows]], axis=0)
        vj = jnp.concatenate([fv[rows], ov[rows]], axis=0)
        s = nt(jnp.concatenate([jnp.where(m, qj, zero) for m in masks], axis=0), kj) * SCALE
        s = jnp.where(same, s, FAR)
        w = jnp.exp2(s - jnp.max(s, axis=1, keepdims=True))
        o = nn(w.astype(BF16), vj) / jnp.sum(w, axis=1, keepdims=True)
        mixed = o[0:64]
        for head in range(1, HEADS):
            mixed = jnp.where(masks[head], o[64 * head:64 * head + 64], mixed)
        mixes.append(mixed.astype(BF16))
    moved = nn(jnp.concatenate(mixes, axis=0), fw_ref[3]).astype(BF16).astype(F32)
    after = (x_ref[...] + moved).astype(BF16)

    for f in range(OWN):
        pack(zs, f, jnp.concatenate([after[64 * j + 16 * f:64 * j + 16 * f + 16] for j in range(RB // 16)], axis=0))
    z_copies = [remote(zs.at[lax.rem(z + d + NZ, OWN)], zr.at[slot], z_send.at[slot], z_recv.at[slot], dz(d))
                for slot, d in ((3, two), (1, 1), (2, -1))]
    for copy in z_copies:
        copy.start()
    zr[0] = zs[lax.rem(z, OWN)]
    for copy in z_copies:
        copy.wait_recv()

    for k in range(NS):
        res[k * RB:(k + 1) * RB, :] = unpack(zr, k).astype(F32)
    n2 = norm(res[...]).astype(BF16)
    keys = jnp.concatenate([n2[k * RB:k * RB + TR] for k in range(NS)], axis=0)
    kbuf[0, 0:KB, :] = keys[:, 0:128]
    kbuf[0, KB:BLOCK, :] = jnp.concatenate([keys[0:KB // 2, 128:E], keys[KB // 2:KB, 128:E]], axis=1)

    low, high = pl.ds(0, HALF), pl.ds(HALF, HALF)

    def send_block(slot, which, target, to_slot, rows, recv):
        src = kbuf.at[slot] if rows is None else kbuf.at[slot, rows]
        dst = kbuf.at[to_slot] if rows is None else kbuf.at[to_slot, rows]
        return remote(src, dst, own_send.at[slot, which], recv.at[to_slot], target)

    def sends(i):
        t, p, a = ORDER[i]
        out = []
        if (p, a) == (0, 0):
            out += [(2, y_pair, SLOT[t, 1, 0], None, ag_recv)]
        if a == 0:
            out += [(0, x_up, SLOT[t, p, 1], None, ag_recv), (1, x_down, SLOT[t, p, 2], None, ag_recv)]
        if a == 1:
            out += [(0, x_up, SLOT[t, p, 3], low, ag_recv)]
        if a == 2:
            out += [(1, x_down, SLOT[t, p, 3], high, ag_recv2)]
        return [send_block(i, *o) for o in out]

    def sib_copy(i):
        return remote(kbuf.at[i], kbuf.at[STEPS + i], sib_send.at[i], sib_recv.at[i], sibling)

    across = remote(kbuf.at[0], kbuf.at[SLOT[1, 0, 0]], far_send.at[0], ag_recv.at[SLOT[1, 0, 0]], dz(4))

    def handle(i):
        t, p, a = ORDER[i]
        if i:
            if a == 3:
                remote(kbuf.at[i, low], kbuf.at[i, low], own_send.at[i, 0], ag_recv.at[i], x_up).wait_recv()
                remote(kbuf.at[i, high], kbuf.at[i, high], own_send.at[i, 0], ag_recv2.at[i], x_up).wait_recv()
            else:
                remote(kbuf.at[i], kbuf.at[i], own_send.at[i, 0], ag_recv.at[i], x_up).wait_recv()
        for copy in sends(i):
            copy.start()
        sib_copy(i).start()

    across.start()
    handle(0)

    fetch[3].wait()
    fetch[4].wait()
    fetch[5].wait()
    q2 = nn(n2, rw_ref[0]).astype(BF16)
    wk = rw_ref[1]
    zero = jnp.zeros((E, E), BF16)
    for g in range(HEADS // 2):
        pair = [(nt(jnp.where(head_mask(E, 2 * g + k), wk, zero), q2) * SCALE).astype(BF16) for k in range(2)]
        pair = jnp.concatenate(pair, axis=1)
        for t in range(3):
            part = pair[:, UW * t:UW * t + UW]
            for k in range(2):
                qp[3 * g + t, k, 0:128, :] = part[0:128]
                qp[3 * g + t, k, 128 + 64 * k:192 + 64 * k, :] = part[128:E]
                qp[3 * g + t, k, 192 - 64 * k:256 - 64 * k, :] = jnp.zeros((64, UW), BF16)
    wvt = nt(eye(E), rw_ref[2]).astype(BF16)
    gap = jnp.zeros((E, 64), BF16)
    wv[0] = jnp.concatenate([wvt, gap], axis=1)
    wv[1] = jnp.concatenate([wvt[:, 0:128], gap, wvt[:, 128:E]], axis=1)
    va[...] = jnp.ones_like(va)
    acc[...] = jnp.zeros_like(acc)
    m_acc[...] = jnp.full_like(m_acc, FAR)
    m_new[...] = jnp.full_like(m_new, FAR)

    span = [(0, 48), (0, 80), (32, 80)]

    def blocks_of(i):
        if isinstance(i, int) and i == 0:
            return 0, STEPS
        one = jnp.where(i < STEPS - 1, i + 1, 2 * STEPS - 1)
        other = jnp.where(i == 1, 1, i + STEPS - 1)
        return (jnp.where(i == 3, STEPS + 3, jnp.where(i == 4, 4, one)), jnp.where(i == 4, 5, other))

    def half_keys(i, k):
        return jnp.concatenate([
            jnp.concatenate([kbuf[slot, 128 * k:128 * k + 128, :], kbuf[slot, KB:BLOCK, :]], axis=1)
            for slot in blocks_of(i)], axis=0)

    def score(i, u):
        for k in range(2):
            s = nn(half_keys(i, k), qp[u, k])
            sbuf[u, KB * k:KB * k + KB, :] = s
            m_new[u] = jnp.maximum(m_new[u], jnp.max(s, axis=0, keepdims=True))

    def weigh(u):
        lo, hi = span[u % 3]
        new = m_new[u]
        fade = jnp.exp2(m_acc[u] - new)
        m_acc[u] = new
        w = jnp.exp2(sbuf[u] - new).astype(BF16)
        acc[u, lo:hi, :] = acc[u, lo:hi, :] * fade + nn(va[u // 3, lo:hi, :], w)

    def values(i):
        for k in range(2):
            vt = nt(wv[k], half_keys(i, k)).astype(BF16)
            for g in range(3):
                va[g, 0:32, KB * k:KB * k + KB] = vt[64 * g:64 * g + 32]
                va[g, 48:80, KB * k:KB * k + KB] = vt[64 * g + 32:64 * g + 64]

    def arrive(i):
        remote(kbuf.at[0], kbuf.at[STEPS + i], sib_send.at[i], sib_recv.at[i], sibling).wait_recv()

    def advance(i, following):
        values(i)
        order = []
        for u in range(UNITS):
            order += [("s", u + 3), ("w", u)]
        seq = []
        for u in range(0, UNITS, 2):
            chunk = [u] + ([u + 1] if u + 1 < UNITS else [])
            seq += [("s", v + 3) for v in chunk] + [("w", v) for v in chunk]
        for kind, u in seq:
            if kind == "w":
                weigh(u)
            elif u < UNITS:
                score(i, u)
            elif following is not None:
                score(following, u - UNITS)

    arrive(0)
    score(0, 0)
    score(0, 1)
    score(0, 2)
    advance(0, None)
    handle(1)
    handle(2)
    score(1, 0)
    score(1, 1)
    score(1, 2)

    def step(i, carry):
        def pick(lo, hi):
            if hi - lo == 1:
                for k in {2: (), 3: (4, 5)}.get(lo, (lo + 2,)):
                    handle(k)
                return
            mid = (lo + hi) // 2
            pl.when(i < mid)(lambda: pick(lo, mid))
            pl.when(i >= mid)(lambda: pick(mid, hi))

        pl.when(i < STEPS - 2)(lambda: pick(1, STEPS - 2))

        @pl.when((i != 3) & (i < STEPS - 1))
        def _():
            arrive(i)

        @pl.when((i == 2) | (i == STEPS - 2))
        def _():
            arrive(i + 1)

        advance(i, jnp.minimum(i + 1, STEPS - 1))
        return carry

    lax.fori_loop(1, STEPS, step, 0)

    parts = []
    for g in range(3):
        o = [acc[3 * g + t] for t in range(3)]
        o = [v / v[32:33] for v in o]
        parts += [jnp.concatenate([o[0][0:32], o[1][0:32, 0:UW // 2]], axis=1),
                  jnp.concatenate([o[1][48:80, UW // 2:], o[2][48:80]], axis=1)]
    mix_t = jnp.concatenate(parts, axis=0).astype(BF16)
    mix = nt(eye(NQ), mix_t).astype(BF16)
    after_row = res[...] + nn(mix, rw_ref[3])
    n3 = norm(after_row).astype(BF16)
    hidden = nn(n3, up_ref[...])
    hidden = (hidden * 0.5 * (1.0 + lax.erf(hidden * (2.0 ** -0.5)))).astype(BF16)
    out = (after_row + nt(hidden, down_ref[...])).astype(BF16)
    for k in range(NS):
        pack(os_ref, k, out[k * RB:(k + 1) * RB])

    mine = lax.rem(z, OWN)
    o_copies = [remote(os_ref.at[slot], or_ref.at[mine], o_send.at[slot], o_recv.at[mine], dz(d))
                for slot, d in ((3, -two), (1, -1), (2, 1))]
    for copy in o_copies:
        copy.start()
    or_ref[mine] = os_ref[0]
    for d in (1, -1, 2):
        f = lax.rem(z + d + NZ, OWN)
        remote(os_ref.at[0], or_ref.at[f], o_send.at[0], o_recv.at[f], sibling).wait_recv()
    blocks = [unpack(or_ref, f) for f in range(OWN)]
    train_out[...] = jnp.concatenate([v[0:TR] for v in blocks], axis=1)
    test_out[...] = jnp.concatenate([v[TR:RB] for v in blocks], axis=1)

    for copy in ex + z_copies + o_copies + [across]:
        copy.wait_send()
    for i in range(STEPS):
        for copy in sends(i):
            copy.wait_send()
        sib_copy(i).wait_send()


def body(*args):
    args = (*args[:5], args[5].T)
    train, test = args[0], args[1]
    dma = pltpu.SemaphoreType.DMA
    return pl.pallas_call(
        kernel,
        name="layer",
        out_shape=(pltpu.VMEM(train.shape, BF16), pltpu.VMEM(test.shape, BF16)),
        in_specs=[pl.BlockSpec(memory_space=pl.ANY)] * 6,
        out_specs=(pl.BlockSpec(memory_space=pltpu.VMEM),) * 2,
        scratch_shapes=[pltpu.VMEM(v.shape, BF16) for v in args] + [
            pltpu.VMEM((TR, OWN * E), BF16),
            pltpu.VMEM((TE, OWN * E), BF16),
            pltpu.VMEM((OWN * RB, E), F32),
            pltpu.VMEM((OWN * RB, E), F32),
            pltpu.VMEM((OWN, ZB, 128), BF16),
            pltpu.VMEM((NS, ZB, 128), BF16),
            pltpu.VMEM((2 * STEPS, BLOCK, 128), BF16),
            pltpu.VMEM((UNITS, 2, 256, UW), BF16),
            pltpu.VMEM((2, E, 256), BF16),
            pltpu.VMEM((3, 80, 2 * KB), BF16),
            pltpu.VMEM((UNITS, 2 * KB, UW), F32),
            pltpu.VMEM((UNITS, 80, UW), F32),
            pltpu.VMEM((UNITS, 1, UW), F32),
            pltpu.VMEM((UNITS, 1, UW), F32),
            pltpu.VMEM((NS, ZB, 128), BF16),
            pltpu.VMEM((OWN, ZB, 128), BF16),
            pltpu.VMEM((NQ, E), F32),
            dma((2,)), dma((2,)), dma((NS,)), dma((NS,)),
            dma((STEPS, 4)), dma((STEPS,)), dma((STEPS,)), dma((STEPS,)), dma((STEPS,)),
            dma((NS,)), dma((OWN,)), dma((1,)), dma((6,)),
        ],
        compiler_params=pltpu.CompilerParams(
            collective_id=0, has_side_effects=True, vmem_limit_bytes=60 * 1024 * 1024),
    )(*args)


def solution(mesh):
    return jax.shard_map(
        body,
        mesh=mesh,
        in_specs=(P("rows", "feat"), P("rows", "feat"), P(), P(), P(), P()),
        out_specs=(P("rows", "feat"), P("rows", "feat")),
        check_vma=False,
    )
```

```python
import functools

import jax
import jax.numpy as jnp
from jax import lax
from jax.experimental import pallas as pl
from jax.experimental.pallas import tpu as pltpu
from jax.sharding import PartitionSpec as P

E = 192
HEADS = 6
HD = 32
HID = 768
F = 8
EPS = 1e-05
SCALE = HD ** (-0.5) * 1.4426950408889634
FAR = -1e30
MESH = pl.DeviceIdType.MESH
F32 = jnp.float32
BF16 = jnp.bfloat16

NX, NY, NZ, NC = 4, 4, 8, 2
OWN = F // 2
TR, TE = 64, 32
RB = TR + TE
ZB = RB + RB // 2
NS = 4
NQ = NS * RB
KB = NS * TR
BLOCK = KB * 3 // 2
HALF = BLOCK // 2

ORDER = [(0, 0, 0), (0, 1, 0), (0, 0, 1), (0, 0, 2), (0, 1, 1), (0, 1, 2), (1, 0, 0), (0, 0, 3),
         (0, 1, 3), (1, 1, 0), (1, 0, 1), (1, 0, 2), (1, 1, 1), (1, 1, 2), (1, 0, 3), (1, 1, 3)]
SLOT = {pos: i for i, pos in enumerate(ORDER)}
STEPS = len(ORDER)
UW = 256
UNITS = HEADS * NQ // UW


def nt(a, b):
    return lax.dot_general(a, b, (((1,), (1,)), ((), ())), preferred_element_type=F32)


def nn(a, b):
    return lax.dot_general(a, b, (((1,), (0,)), ((), ())), preferred_element_type=F32)


def norm(v):
    centred = v - jnp.mean(v, axis=-1, keepdims=True)
    spread = jnp.mean(centred * centred, axis=-1, keepdims=True)
    return centred * lax.rsqrt(spread + EPS)


def eye(n):
    r = lax.broadcasted_iota(jnp.int32, (n, n), 0)
    c = lax.broadcasted_iota(jnp.int32, (n, n), 1)
    return jnp.where(r == c, 1.0, 0.0).astype(BF16)


def pack(ref, at, v):
    ref[at, 0:RB, :] = v[:, 0:128]
    for lo, n in ((0, TR // 2), (TR, TE // 2)):
        ref[at, RB + lo // 2:RB + lo // 2 + n, :] = jnp.concatenate(
            [v[lo:lo + n, 128:E], v[lo + n:lo + 2 * n, 128:E]], axis=1)


def unpack(ref, at):
    right = []
    for lo, n in ((0, TR // 2), (TR, TE // 2)):
        pair = ref[at, RB + lo // 2:RB + lo // 2 + n, :]
        right += [pair[:, 0:64], pair[:, 64:128]]
    return jnp.concatenate([ref[at, 0:RB, :], jnp.concatenate(right, axis=0)], axis=1)


def head_mask(rows, h):
    lane = lax.broadcasted_iota(jnp.int32, (rows, E), 1)
    return (lane >= h * HD) & (lane < (h + 1) * HD)


def kernel(train_in, test_in, fw_in, rw_in, up_in, down_in,
           train_out, test_out,
           train_ref, test_ref, fw_ref, rw_ref, up_ref, down_ref,
           cell_tr, cell_te, x_ref, x2_ref, zs, zr, kbuf, qp, wv, va, sbuf, acc, m_acc, m_new, os_ref, or_ref, res,
           ex_send, ex_recv, z_send, z_recv, own_send, sib_send, ag_recv, ag_recv2, sib_recv,
           o_send, o_recv, far_send, in_sem):
    r = lax.axis_index("rows")
    h = lax.axis_index("feat")
    c = lax.rem(r, NC)
    z = lax.rem(r // NC, NZ)
    x = lax.rem(r // (NC * NZ), NX)
    ylo = r // (NC * NZ * NX)
    y = h * 2 + ylo

    def dev(x_, y_, z_, c_):
        row = ((lax.rem(y_, 2) * NX + x_) * NZ + z_) * NC + c_
        return {"rows": row, "feat": y_ // 2}

    def dz(d):
        return dev(x, y, lax.rem(z + d + NZ, NZ), c)

    x_up, x_down = dev(lax.rem(x + 1, NX), y, z, c), dev(lax.rem(x + 3, NX), y, z, c)
    y_pair = dev(x, 2 * h + 1 - ylo, z, c)
    sibling = dev(x, y, z, 1 - c)
    partner = dev(x, lax.rem(y + 2, NY), z, c)
    two = jnp.where(lax.rem(z, 2) == 0, 2, -2)

    barrier = pltpu.get_barrier_semaphore()
    peers = (partner, dz(2), dz(-2), dz(1), dz(-1), x_up, x_down, y_pair, sibling)
    for target in peers:
        pl.semaphore_signal(barrier, inc=1, device_id=target, device_id_type=MESH)
    fetch = [pltpu.make_async_copy(a, b, in_sem.at[k]) for k, (a, b) in enumerate((
        (train_in, train_ref), (test_in, test_ref), (fw_in, fw_ref), (rw_in, rw_ref),
        (up_in, up_ref), (down_in, down_ref)))]
    for copy in fetch:
        copy.start()
    fetch[0].wait()
    fetch[1].wait()
    pl.semaphore_wait(barrier, len(peers))

    def remote(src, dst, send, recv, target):
        return pltpu.make_async_remote_copy(src_ref=src, dst_ref=dst, send_sem=send, recv_sem=recv,
                                            device_id=target, device_id_type=MESH)

    ex = [remote(train_ref, cell_tr, ex_send.at[0], ex_recv.at[0], partner),
          remote(test_ref, cell_te, ex_send.at[1], ex_recv.at[1], partner)]
    for copy in ex:
        copy.start()

    def gather(tr, te, to):
        for f in range(OWN):
            for j in range(RB // 16):
                ref, row = (tr, 16 * j) if j < TR // 16 else (te, 16 * j - TR)
                to[64 * j + 16 * f:64 * j + 16 * f + 16, :] = ref[row:row + 16, f * E:(f + 1) * E].astype(F32)

    gather(train_ref, test_ref, x_ref)
    n1 = norm(x_ref[...]).astype(BF16)
    fetch[2].wait()
    fq = nn(n1, fw_ref[0]).astype(BF16)
    fk = nn(n1, fw_ref[1]).astype(BF16)
    fv = nn(n1, fw_ref[2]).astype(BF16)
    for copy in ex:
        copy.wait_recv()
    gather(cell_tr, cell_te, x2_ref)
    n1 = norm(x2_ref[...]).astype(BF16)
    ok = nn(n1, fw_ref[1]).astype(BF16)
    ov = nn(n1, fw_ref[2]).astype(BF16)
    shape = (HEADS * 64, 128)
    same = (lax.rem(lax.broadcasted_iota(jnp.int32, shape, 0), 16)
            == lax.rem(lax.broadcasted_iota(jnp.int32, shape, 1), 16))
    masks = [head_mask(64, head) for head in range(HEADS)]
    zero = jnp.zeros((64, E), BF16)
    mixes = []
    for j in range(RB // 16):
        rows = slice(64 * j, 64 * j + 64)
        qj = fq[rows]
        kj = jnp.concatenate([fk[rows], ok[rows]], axis=0)
        vj = jnp.concatenate([fv[rows], ov[rows]], axis=0)
        s = nt(jnp.concatenate([jnp.where(m, qj, zero) for m in masks], axis=0), kj) * SCALE
        s = jnp.where(same, s, FAR)
        w = jnp.exp2(s - jnp.max(s, axis=1, keepdims=True))
        o = nn(w.astype(BF16), vj) / jnp.sum(w, axis=1, keepdims=True)
        mixed = o[0:64]
        for head in range(1, HEADS):
            mixed = jnp.where(masks[head], o[64 * head:64 * head + 64], mixed)
        mixes.append(mixed.astype(BF16))
    moved = nn(jnp.concatenate(mixes, axis=0), fw_ref[3]).astype(BF16).astype(F32)
    after = (x_ref[...] + moved).astype(BF16)

    for f in range(OWN):
        pack(zs, f, jnp.concatenate([after[64 * j + 16 * f:64 * j + 16 * f + 16] for j in range(RB // 16)], axis=0))
    z_copies = [remote(zs.at[lax.rem(z + d + NZ, OWN)], zr.at[slot], z_send.at[slot], z_recv.at[slot], dz(d))
                for slot, d in ((3, two), (1, 1), (2, -1))]
    for copy in z_copies:
        copy.start()
    zr[0] = zs[lax.rem(z, OWN)]
    for copy in z_copies:
        copy.wait_recv()

    for k in range(NS):
        res[k * RB:(k + 1) * RB, :] = unpack(zr, k).astype(F32)
    n2 = norm(res[...]).astype(BF16)
    keys = jnp.concatenate([n2[k * RB:k * RB + TR] for k in range(NS)], axis=0)
    kbuf[0, 0:KB, :] = keys[:, 0:128]
    kbuf[0, KB:BLOCK, :] = jnp.concatenate([keys[0:KB // 2, 128:E], keys[KB // 2:KB, 128:E]], axis=1)

    low, high = pl.ds(0, HALF), pl.ds(HALF, HALF)

    def send_block(slot, which, target, to_slot, rows, recv):
        src = kbuf.at[slot] if rows is None else kbuf.at[slot, rows]
        dst = kbuf.at[to_slot] if rows is None else kbuf.at[to_slot, rows]
        return remote(src, dst, own_send.at[slot, which], recv.at[to_slot], target)

    def sends(i):
        t, p, a = ORDER[i]
        out = []
        if (p, a) == (0, 0):
            out += [(2, y_pair, SLOT[t, 1, 0], None, ag_recv)]
        if a == 0:
            out += [(0, x_up, SLOT[t, p, 1], None, ag_recv), (1, x_down, SLOT[t, p, 2], None, ag_recv)]
        if a == 1:
            out += [(0, x_up, SLOT[t, p, 3], low, ag_recv)]
        if a == 2:
            out += [(1, x_down, SLOT[t, p, 3], high, ag_recv2)]
        return [send_block(i, *o) for o in out]

    def sib_copy(i):
        return remote(kbuf.at[i], kbuf.at[STEPS + i], sib_send.at[i], sib_recv.at[i], sibling)

    across = remote(kbuf.at[0], kbuf.at[SLOT[1, 0, 0]], far_send.at[0], ag_recv.at[SLOT[1, 0, 0]], dz(4))

    def handle(i):
        t, p, a = ORDER[i]
        if i:
            if a == 3:
                remote(kbuf.at[i, low], kbuf.at[i, low], own_send.at[i, 0], ag_recv.at[i], x_up).wait_recv()
                remote(kbuf.at[i, high], kbuf.at[i, high], own_send.at[i, 0], ag_recv2.at[i], x_up).wait_recv()
            else:
                remote(kbuf.at[i], kbuf.at[i], own_send.at[i, 0], ag_recv.at[i], x_up).wait_recv()
        for copy in sends(i):
            copy.start()
        sib_copy(i).start()

    across.start()
    handle(0)

    fetch[3].wait()
    fetch[4].wait()
    fetch[5].wait()
    q2 = nn(n2, rw_ref[0]).astype(BF16)
    wk = rw_ref[1]
    zero = jnp.zeros((E, E), BF16)
    for g in range(HEADS // 2):
        pair = [(nt(jnp.where(head_mask(E, 2 * g + k), wk, zero), q2) * SCALE).astype(BF16) for k in range(2)]
        pair = jnp.concatenate(pair, axis=1)
        for t in range(3):
            part = pair[:, UW * t:UW * t + UW]
            for k in range(2):
                qp[3 * g + t, k, 0:128, :] = part[0:128]
                qp[3 * g + t, k, 128 + 64 * k:192 + 64 * k, :] = part[128:E]
                qp[3 * g + t, k, 192 - 64 * k:256 - 64 * k, :] = jnp.zeros((64, UW), BF16)
    wvt = nt(eye(E), rw_ref[2]).astype(BF16)
    gap = jnp.zeros((E, 64), BF16)
    wv[0] = jnp.concatenate([wvt, gap], axis=1)
    wv[1] = jnp.concatenate([wvt[:, 0:128], gap, wvt[:, 128:E]], axis=1)
    va[...] = jnp.ones_like(va)
    acc[...] = jnp.zeros_like(acc)
    m_acc[...] = jnp.full_like(m_acc, FAR)
    m_new[...] = jnp.full_like(m_new, FAR)

    span = [(0, 48), (0, 80), (32, 80)]

    def blocks_of(i):
        if isinstance(i, int) and i == 0:
            return 0, STEPS
        one = jnp.where(i < STEPS - 1, i + 1, 2 * STEPS - 1)
        other = jnp.where(i == 1, 1, i + STEPS - 1)
        return (jnp.where(i == 3, STEPS + 3, jnp.where(i == 4, 4, one)), jnp.where(i == 4, 5, other))

    def half_keys(i, k):
        return jnp.concatenate([
            jnp.concatenate([kbuf[slot, 128 * k:128 * k + 128, :], kbuf[slot, KB:BLOCK, :]], axis=1)
            for slot in blocks_of(i)], axis=0)

    def score(i, u):
        for k in range(2):
            s = nn(half_keys(i, k), qp[u, k])
            sbuf[u, KB * k:KB * k + KB, :] = s
            m_new[u] = jnp.maximum(m_new[u], jnp.max(s, axis=0, keepdims=True))

    def weigh(u):
        lo, hi = span[u % 3]
        new = m_new[u]
        fade = jnp.exp2(m_acc[u] - new)
        m_acc[u] = new
        w = jnp.exp2(sbuf[u] - new).astype(BF16)
        acc[u, lo:hi, :] = acc[u, lo:hi, :] * fade + nn(va[u // 3, lo:hi, :], w)

    def values(i):
        for k in range(2):
            vt = nt(wv[k], half_keys(i, k)).astype(BF16)
            for g in range(3):
                va[g, 0:32, KB * k:KB * k + KB] = vt[64 * g:64 * g + 32]
                va[g, 48:80, KB * k:KB * k + KB] = vt[64 * g + 32:64 * g + 64]

    def arrive(i):
        remote(kbuf.at[0], kbuf.at[STEPS + i], sib_send.at[i], sib_recv.at[i], sibling).wait_recv()

    def advance(i, following):
        values(i)
        for u in range(UNITS):
            if u + 3 < UNITS:
                score(i, u + 3)
            elif following is not None:
                score(following, u + 3 - UNITS)
            weigh(u)

    arrive(0)
    score(0, 0)
    score(0, 1)
    score(0, 2)
    advance(0, None)
    handle(1)
    handle(2)
    score(1, 0)
    score(1, 1)
    score(1, 2)

    def step(i, carry):
        def pick(lo, hi):
            if hi - lo == 1:
                for k in {2: (), 3: (4, 5)}.get(lo, (lo + 2,)):
                    handle(k)
                return
            mid = (lo + hi) // 2
            pl.when(i < mid)(lambda: pick(lo, mid))
            pl.when(i >= mid)(lambda: pick(mid, hi))

        pl.when(i < STEPS - 2)(lambda: pick(1, STEPS - 2))

        @pl.when((i != 3) & (i < STEPS - 1))
        def _():
            arrive(i)

        @pl.when((i == 2) | (i == STEPS - 2))
        def _():
            arrive(i + 1)

        advance(i, jnp.minimum(i + 1, STEPS - 1))
        return carry

    lax.fori_loop(1, STEPS, step, 0)

    parts = []
    for g in range(3):
        o = [acc[3 * g + t] for t in range(3)]
        o = [v / v[32:33] for v in o]
        parts += [jnp.concatenate([o[0][0:32], o[1][0:32, 0:UW // 2]], axis=1),
                  jnp.concatenate([o[1][48:80, UW // 2:], o[2][48:80]], axis=1)]
    mix_t = jnp.concatenate(parts, axis=0).astype(BF16)
    mix = nt(eye(NQ), mix_t).astype(BF16)
    after_row = res[...] + nn(mix, rw_ref[3])
    n3 = norm(after_row).astype(BF16)
    hidden = nn(n3, up_ref[...])
    hidden = (hidden * 0.5 * (1.0 + lax.erf(hidden * (2.0 ** -0.5)))).astype(BF16)
    out = (after_row + nt(hidden, down_ref[...])).astype(BF16)
    for k in range(NS):
        pack(os_ref, k, out[k * RB:(k + 1) * RB])

    mine = lax.rem(z, OWN)
    o_copies = [remote(os_ref.at[slot], or_ref.at[mine], o_send.at[slot], o_recv.at[mine], dz(d))
                for slot, d in ((3, -two), (1, -1), (2, 1))]
    for copy in o_copies:
        copy.start()
    or_ref[mine] = os_ref[0]
    for d in (1, -1, 2):
        f = lax.rem(z + d + NZ, OWN)
        remote(os_ref.at[0], or_ref.at[f], o_send.at[0], o_recv.at[f], sibling).wait_recv()
    blocks = [unpack(or_ref, f) for f in range(OWN)]
    train_out[...] = jnp.concatenate([v[0:TR] for v in blocks], axis=1)
    test_out[...] = jnp.concatenate([v[TR:RB] for v in blocks], axis=1)

    for copy in ex + z_copies + o_copies + [across]:
        copy.wait_send()
    for i in range(STEPS):
        for copy in sends(i):
            copy.wait_send()
        sib_copy(i).wait_send()


def body(*args):
    args = (*args[:5], args[5].T)
    train, test = args[0], args[1]
    dma = pltpu.SemaphoreType.DMA
    return pl.pallas_call(
        kernel,
        name="layer",
        out_shape=(pltpu.VMEM(train.shape, BF16), pltpu.VMEM(test.shape, BF16)),
        in_specs=[pl.BlockSpec(memory_space=pl.ANY)] * 6,
        out_specs=(pl.BlockSpec(memory_space=pltpu.VMEM),) * 2,
        scratch_shapes=[pltpu.VMEM(v.shape, BF16) for v in args] + [
            pltpu.VMEM((TR, OWN * E), BF16),
            pltpu.VMEM((TE, OWN * E), BF16),
            pltpu.VMEM((OWN * RB, E), F32),
            pltpu.VMEM((OWN * RB, E), F32),
            pltpu.VMEM((OWN, ZB, 128), BF16),
            pltpu.VMEM((NS, ZB, 128), BF16),
            pltpu.VMEM((2 * STEPS, BLOCK, 128), BF16),
            pltpu.VMEM((UNITS, 2, 256, UW), BF16),
            pltpu.VMEM((2, E, 256), BF16),
            pltpu.VMEM((3, 80, 2 * KB), BF16),
            pltpu.VMEM((UNITS, 2 * KB, UW), F32),
            pltpu.VMEM((UNITS, 80, UW), F32),
            pltpu.VMEM((UNITS, 1, UW), F32),
            pltpu.VMEM((UNITS, 1, UW), F32),
            pltpu.VMEM((NS, ZB, 128), BF16),
            pltpu.VMEM((OWN, ZB, 128), BF16),
            pltpu.VMEM((NQ, E), F32),
            dma((2,)), dma((2,)), dma((NS,)), dma((NS,)),
            dma((STEPS, 4)), dma((STEPS,)), dma((STEPS,)), dma((STEPS,)), dma((STEPS,)),
            dma((NS,)), dma((OWN,)), dma((1,)), dma((6,)),
        ],
        compiler_params=pltpu.CompilerParams(
            collective_id=0, has_side_effects=True, vmem_limit_bytes=60 * 1024 * 1024),
    )(*args)


def solution(mesh):
    return jax.shard_map(
        body,
        mesh=mesh,
        in_specs=(P("rows", "feat"), P("rows", "feat"), P(), P(), P(), P()),
        out_specs=(P("rows", "feat"), P("rows", "feat")),
        check_vma=False,
    )
```

```python
import functools

import jax
import jax.numpy as jnp
from jax import lax
from jax.experimental import pallas as pl
from jax.experimental.pallas import tpu as pltpu
from jax.sharding import PartitionSpec as P

E = 192
HEADS = 6
HD = 32
HID = 768
F = 8
EPS = 1e-05
SCALE = HD ** (-0.5) * 1.4426950408889634
FAR = -1e30
MESH = pl.DeviceIdType.MESH
F32 = jnp.float32
BF16 = jnp.bfloat16

NX, NY, NZ, NC = 4, 4, 8, 2
OWN = F // 2
TR, TE = 64, 32
RB = TR + TE
ZB = RB + RB // 2
NS = 4
NQ = NS * RB
KB = NS * TR
BLOCK = KB * 3 // 2
HALF = BLOCK // 2

ORDER = [(0, 0, 0), (0, 1, 0), (0, 0, 1), (0, 0, 2), (0, 1, 1), (0, 1, 2), (1, 0, 0), (0, 0, 3),
         (0, 1, 3), (1, 1, 0), (1, 0, 1), (1, 0, 2), (1, 1, 1), (1, 1, 2), (1, 0, 3), (1, 1, 3)]
SLOT = {pos: i for i, pos in enumerate(ORDER)}
STEPS = len(ORDER)
UW = 256
UNITS = HEADS * NQ // UW


def nt(a, b):
    return lax.dot_general(a, b, (((1,), (1,)), ((), ())), preferred_element_type=F32)


def nn(a, b):
    return lax.dot_general(a, b, (((1,), (0,)), ((), ())), preferred_element_type=F32)


def norm(v):
    centred = v - jnp.mean(v, axis=-1, keepdims=True)
    spread = jnp.mean(centred * centred, axis=-1, keepdims=True)
    return centred * lax.rsqrt(spread + EPS)


def eye(n):
    r = lax.broadcasted_iota(jnp.int32, (n, n), 0)
    c = lax.broadcasted_iota(jnp.int32, (n, n), 1)
    return jnp.where(r == c, 1.0, 0.0).astype(BF16)


def pack(ref, at, v):
    ref[at, 0:RB, :] = v[:, 0:128]
    for lo, n in ((0, TR // 2), (TR, TE // 2)):
        ref[at, RB + lo // 2:RB + lo // 2 + n, :] = jnp.concatenate(
            [v[lo:lo + n, 128:E], v[lo + n:lo + 2 * n, 128:E]], axis=1)


def unpack(ref, at):
    right = []
    for lo, n in ((0, TR // 2), (TR, TE // 2)):
        pair = ref[at, RB + lo // 2:RB + lo // 2 + n, :]
        right += [pair[:, 0:64], pair[:, 64:128]]
    return jnp.concatenate([ref[at, 0:RB, :], jnp.concatenate(right, axis=0)], axis=1)


def head_mask(rows, h):
    lane = lax.broadcasted_iota(jnp.int32, (rows, E), 1)
    return (lane >= h * HD) & (lane < (h + 1) * HD)


def kernel(train_in, test_in, fw_in, rw_in, up_in, down_in,
           train_out, test_out,
           train_ref, test_ref, fw_ref, rw_ref, up_ref, down_ref,
           cell_tr, cell_te, x_ref, x2_ref, zs, zr, kbuf, qp, wv, va, sbuf, acc, m_acc, m_new, os_ref, or_ref, res,
           ex_send, ex_recv, z_send, z_recv, own_send, sib_send, ag_recv, ag_recv2, sib_recv,
           o_send, o_recv, far_send, in_sem):
    r = lax.axis_index("rows")
    h = lax.axis_index("feat")
    c = lax.rem(r, NC)
    z = lax.rem(r // NC, NZ)
    x = lax.rem(r // (NC * NZ), NX)
    ylo = r // (NC * NZ * NX)
    y = h * 2 + ylo

    def dev(x_, y_, z_, c_):
        row = ((lax.rem(y_, 2) * NX + x_) * NZ + z_) * NC + c_
        return {"rows": row, "feat": y_ // 2}

    def dz(d):
        return dev(x, y, lax.rem(z + d + NZ, NZ), c)

    x_up, x_down = dev(lax.rem(x + 1, NX), y, z, c), dev(lax.rem(x + 3, NX), y, z, c)
    y_pair = dev(x, 2 * h + 1 - ylo, z, c)
    sibling = dev(x, y, z, 1 - c)
    partner = dev(x, lax.rem(y + 2, NY), z, c)
    two = jnp.where(lax.rem(z, 2) == 0, 2, -2)

    barrier = pltpu.get_barrier_semaphore()
    peers = (partner, dz(2), dz(-2), dz(1), dz(-1), x_up, x_down, y_pair, sibling)
    for target in peers:
        pl.semaphore_signal(barrier, inc=1, device_id=target, device_id_type=MESH)
    fetch = [pltpu.make_async_copy(a, b, in_sem.at[k]) for k, (a, b) in enumerate((
        (train_in, train_ref), (test_in, test_ref), (fw_in, fw_ref), (rw_in, rw_ref),
        (up_in, up_ref), (down_in, down_ref)))]
    for copy in fetch:
        copy.start()
    fetch[0].wait()
    fetch[1].wait()
    pl.semaphore_wait(barrier, len(peers))

    def remote(src, dst, send, recv, target):
        return pltpu.make_async_remote_copy(src_ref=src, dst_ref=dst, send_sem=send, recv_sem=recv,
                                            device_id=target, device_id_type=MESH)

    ex = [remote(train_ref, cell_tr, ex_send.at[0], ex_recv.at[0], partner),
          remote(test_ref, cell_te, ex_send.at[1], ex_recv.at[1], partner)]
    for copy in ex:
        copy.start()

    def gather(tr, te, to):
        for f in range(OWN):
            for j in range(RB // 16):
                ref, row = (tr, 16 * j) if j < TR // 16 else (te, 16 * j - TR)
                to[64 * j + 16 * f:64 * j + 16 * f + 16, :] = ref[row:row + 16, f * E:(f + 1) * E].astype(F32)

    gather(train_ref, test_ref, x_ref)
    n1 = norm(x_ref[...]).astype(BF16)
    fetch[2].wait()
    fq = nn(n1, fw_ref[0]).astype(BF16)
    fk = nn(n1, fw_ref[1]).astype(BF16)
    fv = nn(n1, fw_ref[2]).astype(BF16)
    for copy in ex:
        copy.wait_recv()
    gather(cell_tr, cell_te, x2_ref)
    n1 = norm(x2_ref[...]).astype(BF16)
    ok = nn(n1, fw_ref[1]).astype(BF16)
    ov = nn(n1, fw_ref[2]).astype(BF16)
    shape = (HEADS * 64, 128)
    same = (lax.rem(lax.broadcasted_iota(jnp.int32, shape, 0), 16)
            == lax.rem(lax.broadcasted_iota(jnp.int32, shape, 1), 16))
    masks = [head_mask(64, head) for head in range(HEADS)]
    zero = jnp.zeros((64, E), BF16)
    mixes = []
    for j in range(RB // 16):
        rows = slice(64 * j, 64 * j + 64)
        qj = fq[rows]
        kj = jnp.concatenate([fk[rows], ok[rows]], axis=0)
        vj = jnp.concatenate([fv[rows], ov[rows]], axis=0)
        s = nt(jnp.concatenate([jnp.where(m, qj, zero) for m in masks], axis=0), kj) * SCALE
        s = jnp.where(same, s, FAR)
        w = jnp.exp2(s - jnp.max(s, axis=1, keepdims=True))
        o = nn(w.astype(BF16), vj) / jnp.sum(w, axis=1, keepdims=True)
        mixed = o[0:64]
        for head in range(1, HEADS):
            mixed = jnp.where(masks[head], o[64 * head:64 * head + 64], mixed)
        mixes.append(mixed.astype(BF16))
    moved = nn(jnp.concatenate(mixes, axis=0), fw_ref[3]).astype(BF16).astype(F32)
    after = x_ref[...] + moved
    normed = norm(after).astype(BF16)

    def rows_of(v, f):
        return jnp.concatenate([v[64 * j + 16 * f:64 * j + 16 * f + 16] for j in range(RB // 16)], axis=0)

    for f in range(OWN):
        pack(zs, f, rows_of(normed, f))
        res[f * RB:(f + 1) * RB, :] = rows_of(after, f)
    z_copies = [remote(zs.at[lax.rem(z + d + NZ, OWN)], zr.at[slot], z_send.at[slot], z_recv.at[slot], dz(d))
                for slot, d in ((3, two), (1, 1), (2, -1))]
    for copy in z_copies:
        copy.start()
    zr[0] = zs[lax.rem(z, OWN)]
    for copy in z_copies:
        copy.wait_recv()

    n2 = jnp.concatenate([unpack(zr, k) for k in range(NS)], axis=0)
    keys = jnp.concatenate([n2[k * RB:k * RB + TR] for k in range(NS)], axis=0)
    kbuf[0, 0:KB, :] = keys[:, 0:128]
    kbuf[0, KB:BLOCK, :] = jnp.concatenate([keys[0:KB // 2, 128:E], keys[KB // 2:KB, 128:E]], axis=1)

    low, high = pl.ds(0, HALF), pl.ds(HALF, HALF)

    def send_block(slot, which, target, to_slot, rows, recv):
        src = kbuf.at[slot] if rows is None else kbuf.at[slot, rows]
        dst = kbuf.at[to_slot] if rows is None else kbuf.at[to_slot, rows]
        return remote(src, dst, own_send.at[slot, which], recv.at[to_slot], target)

    def sends(i):
        t, p, a = ORDER[i]
        out = []
        if (p, a) == (0, 0):
            out += [(2, y_pair, SLOT[t, 1, 0], None, ag_recv)]
        if a == 0:
            out += [(0, x_up, SLOT[t, p, 1], None, ag_recv), (1, x_down, SLOT[t, p, 2], None, ag_recv)]
        if a == 1:
            out += [(0, x_up, SLOT[t, p, 3], low, ag_recv)]
        if a == 2:
            out += [(1, x_down, SLOT[t, p, 3], high, ag_recv2)]
        return [send_block(i, *o) for o in out]

    def sib_copy(i):
        return remote(kbuf.at[i], kbuf.at[STEPS + i], sib_send.at[i], sib_recv.at[i], sibling)

    across = remote(kbuf.at[0], kbuf.at[SLOT[1, 0, 0]], far_send.at[0], ag_recv.at[SLOT[1, 0, 0]], dz(4))

    def handle(i):
        t, p, a = ORDER[i]
        if i:
            if a == 3:
                remote(kbuf.at[i, low], kbuf.at[i, low], own_send.at[i, 0], ag_recv.at[i], x_up).wait_recv()
                remote(kbuf.at[i, high], kbuf.at[i, high], own_send.at[i, 0], ag_recv2.at[i], x_up).wait_recv()
            else:
                remote(kbuf.at[i], kbuf.at[i], own_send.at[i, 0], ag_recv.at[i], x_up).wait_recv()
        for copy in sends(i):
            copy.start()
        sib_copy(i).start()

    across.start()
    handle(0)

    fetch[3].wait()
    fetch[4].wait()
    fetch[5].wait()
    q2 = nn(n2, rw_ref[0]).astype(BF16)
    wk = rw_ref[1]
    zero = jnp.zeros((E, E), BF16)
    for g in range(HEADS // 2):
        pair = [(nt(jnp.where(head_mask(E, 2 * g + k), wk, zero), q2) * SCALE).astype(BF16) for k in range(2)]
        pair = jnp.concatenate(pair, axis=1)
        for t in range(3):
            part = pair[:, UW * t:UW * t + UW]
            for k in range(2):
                qp[3 * g + t, k, 0:128, :] = part[0:128]
                qp[3 * g + t, k, 128 + 64 * k:192 + 64 * k, :] = part[128:E]
                qp[3 * g + t, k, 192 - 64 * k:256 - 64 * k, :] = jnp.zeros((64, UW), BF16)
    wvt = nt(eye(E), rw_ref[2]).astype(BF16)
    gap = jnp.zeros((E, 64), BF16)
    wv[0] = jnp.concatenate([wvt, gap], axis=1)
    wv[1] = jnp.concatenate([wvt[:, 0:128], gap, wvt[:, 128:E]], axis=1)
    va[...] = jnp.ones_like(va)
    acc[...] = jnp.zeros_like(acc)
    m_acc[...] = jnp.full_like(m_acc, FAR)
    m_new[...] = jnp.full_like(m_new, FAR)

    span = [(0, 48), (0, 80), (32, 80)]

    def blocks_of(i):
        if isinstance(i, int) and i == 0:
            return 0, STEPS
        one = jnp.where(i < STEPS - 1, i + 1, 2 * STEPS - 1)
        other = jnp.where(i == 1, 1, i + STEPS - 1)
        return (jnp.where(i == 3, STEPS + 3, jnp.where(i == 4, 4, one)), jnp.where(i == 4, 5, other))

    def half_keys(i, k):
        return jnp.concatenate([
            jnp.concatenate([kbuf[slot, 128 * k:128 * k + 128, :], kbuf[slot, KB:BLOCK, :]], axis=1)
            for slot in blocks_of(i)], axis=0)

    def score(i, u):
        for k in range(2):
            s = nn(half_keys(i, k), qp[u, k])
            sbuf[u, KB * k:KB * k + KB, :] = s
            m_new[u] = jnp.maximum(m_new[u], jnp.max(s, axis=0, keepdims=True))

    def weigh(u):
        lo, hi = span[u % 3]
        new = m_new[u]
        fade = jnp.exp2(m_acc[u] - new)
        m_acc[u] = new
        w = jnp.exp2(sbuf[u] - new).astype(BF16)
        acc[u, lo:hi, :] = acc[u, lo:hi, :] * fade + nn(va[u // 3, lo:hi, :], w)

    def values(i):
        for k in range(2):
            vt = nt(wv[k], half_keys(i, k)).astype(BF16)
            for g in range(3):
                va[g, 0:32, KB * k:KB * k + KB] = vt[64 * g:64 * g + 32]
                va[g, 48:80, KB * k:KB * k + KB] = vt[64 * g + 32:64 * g + 64]

    def arrive(i):
        remote(kbuf.at[0], kbuf.at[STEPS + i], sib_send.at[i], sib_recv.at[i], sibling).wait_recv()

    def advance(i, following):
        values(i)
        for u in range(UNITS):
            if u + 3 < UNITS:
                score(i, u + 3)
            elif following is not None:
                score(following, u + 3 - UNITS)
            weigh(u)

    arrive(0)
    score(0, 0)
    score(0, 1)
    score(0, 2)
    advance(0, None)
    handle(1)
    handle(2)
    score(1, 0)
    score(1, 1)
    score(1, 2)

    def step(i, carry):
        def pick(lo, hi):
            if hi - lo == 1:
                for k in {2: (), 3: (4, 5)}.get(lo, (lo + 2,)):
                    handle(k)
                return
            mid = (lo + hi) // 2
            pl.when(i < mid)(lambda: pick(lo, mid))
            pl.when(i >= mid)(lambda: pick(mid, hi))

        pl.when(i < STEPS - 2)(lambda: pick(1, STEPS - 2))

        @pl.when((i != 3) & (i < STEPS - 1))
        def _():
            arrive(i)

        @pl.when((i == 2) | (i == STEPS - 2))
        def _():
            arrive(i + 1)

        advance(i, jnp.minimum(i + 1, STEPS - 1))
        return carry

    lax.fori_loop(1, STEPS, step, 0)

    parts = []
    for g in range(3):
        o = [acc[3 * g + t] for t in range(3)]
        o = [v / v[32:33] for v in o]
        parts += [jnp.concatenate([o[0][0:32], o[1][0:32, 0:UW // 2]], axis=1),
                  jnp.concatenate([o[1][48:80, UW // 2:], o[2][48:80]], axis=1)]
    mix_t = jnp.concatenate(parts, axis=0).astype(BF16)
    mix = nt(eye(NQ), mix_t).astype(BF16)
    for k in range(NS):
        pack(os_ref, k, mix[k * RB:(k + 1) * RB])

    mine = lax.rem(z, OWN)
    o_copies = [remote(os_ref.at[slot], or_ref.at[mine], o_send.at[slot], o_recv.at[mine], dz(d))
                for slot, d in ((3, -two), (1, -1), (2, 1))]
    for copy in o_copies:
        copy.start()
    or_ref[mine] = os_ref[0]
    for d in (1, -1, 2):
        f = lax.rem(z + d + NZ, OWN)
        remote(os_ref.at[0], or_ref.at[f], o_send.at[0], o_recv.at[f], sibling).wait_recv()
    mix = jnp.concatenate([unpack(or_ref, f) for f in range(OWN)], axis=0)
    after_row = res[...] + nn(mix, rw_ref[3])
    n3 = norm(after_row).astype(BF16)
    hidden = nn(n3, up_ref[...])
    hidden = (hidden * 0.5 * (1.0 + lax.erf(hidden * (2.0 ** -0.5)))).astype(BF16)
    out = (after_row + nt(hidden, down_ref[...])).astype(BF16)
    blocks = [out[f * RB:(f + 1) * RB] for f in range(OWN)]
    train_out[...] = jnp.concatenate([v[0:TR] for v in blocks], axis=1)
    test_out[...] = jnp.concatenate([v[TR:RB] for v in blocks], axis=1)

    for copy in ex + z_copies + o_copies + [across]:
        copy.wait_send()
    for i in range(STEPS):
        for copy in sends(i):
            copy.wait_send()
        sib_copy(i).wait_send()


def body(*args):
    args = (*args[:5], args[5].T)
    train, test = args[0], args[1]
    dma = pltpu.SemaphoreType.DMA
    return pl.pallas_call(
        kernel,
        name="layer",
        out_shape=(pltpu.VMEM(train.shape, BF16), pltpu.VMEM(test.shape, BF16)),
        in_specs=[pl.BlockSpec(memory_space=pl.ANY)] * 6,
        out_specs=(pl.BlockSpec(memory_space=pltpu.VMEM),) * 2,
        scratch_shapes=[pltpu.VMEM(v.shape, BF16) for v in args] + [
            pltpu.VMEM((TR, OWN * E), BF16),
            pltpu.VMEM((TE, OWN * E), BF16),
            pltpu.VMEM((OWN * RB, E), F32),
            pltpu.VMEM((OWN * RB, E), F32),
            pltpu.VMEM((OWN, ZB, 128), BF16),
            pltpu.VMEM((NS, ZB, 128), BF16),
            pltpu.VMEM((2 * STEPS, BLOCK, 128), BF16),
            pltpu.VMEM((UNITS, 2, 256, UW), BF16),
            pltpu.VMEM((2, E, 256), BF16),
            pltpu.VMEM((3, 80, 2 * KB), BF16),
            pltpu.VMEM((UNITS, 2 * KB, UW), F32),
            pltpu.VMEM((UNITS, 80, UW), F32),
            pltpu.VMEM((UNITS, 1, UW), F32),
            pltpu.VMEM((UNITS, 1, UW), F32),
            pltpu.VMEM((NS, ZB, 128), BF16),
            pltpu.VMEM((OWN, ZB, 128), BF16),
            pltpu.VMEM((NQ, E), F32),
            dma((2,)), dma((2,)), dma((NS,)), dma((NS,)),
            dma((STEPS, 4)), dma((STEPS,)), dma((STEPS,)), dma((STEPS,)), dma((STEPS,)),
            dma((NS,)), dma((OWN,)), dma((1,)), dma((6,)),
        ],
        compiler_params=pltpu.CompilerParams(
            collective_id=0, has_side_effects=True, vmem_limit_bytes=60 * 1024 * 1024),
    )(*args)


def solution(mesh):
    return jax.shard_map(
        body,
        mesh=mesh,
        in_specs=(P("rows", "feat"), P("rows", "feat"), P(), P(), P(), P()),
        out_specs=(P("rows", "feat"), P("rows", "feat")),
        check_vma=False,
    )
```

```python
import functools

import jax
import jax.numpy as jnp
from jax import lax
from jax.experimental import pallas as pl
from jax.experimental.pallas import tpu as pltpu
from jax.sharding import PartitionSpec as P

E = 192
HEADS = 6
HD = 32
HID = 768
F = 8
EPS = 1e-05
SCALE = HD ** (-0.5) * 1.4426950408889634
FAR = -1e30
MESH = pl.DeviceIdType.MESH
F32 = jnp.float32
BF16 = jnp.bfloat16

NX, NY, NZ, NC = 4, 4, 8, 2
OWN = F // 2
TR, TE = 64, 32
RB = TR + TE
ZB = RB + RB // 2
NS = 4
NQ = NS * RB
KB = NS * TR
BLOCK = KB * 3 // 2
HALF = BLOCK // 2

ORDER = [(0, 0, 0), (0, 1, 0), (0, 0, 1), (0, 0, 2), (0, 1, 1), (0, 1, 2), (1, 0, 0), (0, 0, 3),
         (0, 1, 3), (1, 1, 0), (1, 0, 1), (1, 0, 2), (1, 1, 1), (1, 1, 2), (1, 0, 3), (1, 1, 3)]
SLOT = {pos: i for i, pos in enumerate(ORDER)}
STEPS = len(ORDER)
UW = 256
UNITS = HEADS * NQ // UW


def nt(a, b):
    return lax.dot_general(a, b, (((1,), (1,)), ((), ())), preferred_element_type=F32)


def nn(a, b):
    return lax.dot_general(a, b, (((1,), (0,)), ((), ())), preferred_element_type=F32)


def norm(v):
    centred = v - jnp.mean(v, axis=-1, keepdims=True)
    spread = jnp.mean(centred * centred, axis=-1, keepdims=True)
    return centred * lax.rsqrt(spread + EPS)


def eye(n):
    r = lax.broadcasted_iota(jnp.int32, (n, n), 0)
    c = lax.broadcasted_iota(jnp.int32, (n, n), 1)
    return jnp.where(r == c, 1.0, 0.0).astype(BF16)


def pack(ref, at, v):
    ref[at, 0:RB, :] = v[:, 0:128]
    for lo, n in ((0, TR // 2), (TR, TE // 2)):
        ref[at, RB + lo // 2:RB + lo // 2 + n, :] = jnp.concatenate(
            [v[lo:lo + n, 128:E], v[lo + n:lo + 2 * n, 128:E]], axis=1)


def unpack(ref, at):
    right = []
    for lo, n in ((0, TR // 2), (TR, TE // 2)):
        pair = ref[at, RB + lo // 2:RB + lo // 2 + n, :]
        right += [pair[:, 0:64], pair[:, 64:128]]
    return jnp.concatenate([ref[at, 0:RB, :], jnp.concatenate(right, axis=0)], axis=1)


def head_mask(rows, h):
    lane = lax.broadcasted_iota(jnp.int32, (rows, E), 1)
    return (lane >= h * HD) & (lane < (h + 1) * HD)


def kernel(train_in, test_in, fw_in, rw_in, up_in, down_in,
           train_out, test_out,
           train_ref, test_ref, fw_ref, rw_ref, up_ref, down_ref,
           cell_tr, cell_te, x_ref, x2_ref, zs, zr, kbuf, qp, wv, va, sbuf, acc, m_acc, m_new, os_ref, or_ref, res, fin,
           ex_send, ex_recv, z_send, z_recv, own_send, sib_send, ag_recv, ag_recv2, sib_recv,
           o_send, o_recv, far_send, in_sem):
    r = lax.axis_index("rows")
    h = lax.axis_index("feat")
    c = lax.rem(r, NC)
    z = lax.rem(r // NC, NZ)
    x = lax.rem(r // (NC * NZ), NX)
    ylo = r // (NC * NZ * NX)
    y = h * 2 + ylo

    def dev(x_, y_, z_, c_):
        row = ((lax.rem(y_, 2) * NX + x_) * NZ + z_) * NC + c_
        return {"rows": row, "feat": y_ // 2}

    def dz(d):
        return dev(x, y, lax.rem(z + d + NZ, NZ), c)

    x_up, x_down = dev(lax.rem(x + 1, NX), y, z, c), dev(lax.rem(x + 3, NX), y, z, c)
    y_pair = dev(x, 2 * h + 1 - ylo, z, c)
    sibling = dev(x, y, z, 1 - c)
    partner = dev(x, lax.rem(y + 2, NY), z, c)
    two = jnp.where(lax.rem(z, 2) == 0, 2, -2)

    barrier = pltpu.get_barrier_semaphore()
    peers = (partner, dz(2), dz(-2), dz(1), dz(-1), x_up, x_down, y_pair, sibling)
    for target in peers:
        pl.semaphore_signal(barrier, inc=1, device_id=target, device_id_type=MESH)
    fetch = [pltpu.make_async_copy(a, b, in_sem.at[k]) for k, (a, b) in enumerate((
        (train_in, train_ref), (test_in, test_ref), (fw_in, fw_ref), (rw_in, rw_ref),
        (up_in, up_ref), (down_in, down_ref)))]
    for copy in fetch:
        copy.start()
    fetch[0].wait()
    fetch[1].wait()
    pl.semaphore_wait(barrier, len(peers))

    def remote(src, dst, send, recv, target):
        return pltpu.make_async_remote_copy(src_ref=src, dst_ref=dst, send_sem=send, recv_sem=recv,
                                            device_id=target, device_id_type=MESH)

    ex = [remote(train_ref, cell_tr, ex_send.at[0], ex_recv.at[0], partner),
          remote(test_ref, cell_te, ex_send.at[1], ex_recv.at[1], partner)]
    for copy in ex:
        copy.start()

    def gather(tr, te, to):
        for f in range(OWN):
            for j in range(RB // 16):
                ref, row = (tr, 16 * j) if j < TR // 16 else (te, 16 * j - TR)
                to[64 * j + 16 * f:64 * j + 16 * f + 16, :] = ref[row:row + 16, f * E:(f + 1) * E].astype(F32)

    gather(train_ref, test_ref, x_ref)
    n1 = norm(x_ref[...]).astype(BF16)
    fetch[2].wait()
    fq = nn(n1, fw_ref[0]).astype(BF16)
    fk = nn(n1, fw_ref[1]).astype(BF16)
    fv = nn(n1, fw_ref[2]).astype(BF16)
    for copy in ex:
        copy.wait_recv()
    gather(cell_tr, cell_te, x2_ref)
    n1 = norm(x2_ref[...]).astype(BF16)
    ok = nn(n1, fw_ref[1]).astype(BF16)
    ov = nn(n1, fw_ref[2]).astype(BF16)
    shape = (HEADS * 64, 128)
    same = (lax.rem(lax.broadcasted_iota(jnp.int32, shape, 0), 16)
            == lax.rem(lax.broadcasted_iota(jnp.int32, shape, 1), 16))
    masks = [head_mask(64, head) for head in range(HEADS)]
    zero = jnp.zeros((64, E), BF16)
    mixes = []
    for j in range(RB // 16):
        rows = slice(64 * j, 64 * j + 64)
        qj = fq[rows]
        kj = jnp.concatenate([fk[rows], ok[rows]], axis=0)
        vj = jnp.concatenate([fv[rows], ov[rows]], axis=0)
        s = nt(jnp.concatenate([jnp.where(m, qj, zero) for m in masks], axis=0), kj) * SCALE
        s = jnp.where(same, s, FAR)
        w = jnp.exp2(s - jnp.max(s, axis=1, keepdims=True))
        o = nn(w.astype(BF16), vj) / jnp.sum(w, axis=1, keepdims=True)
        mixed = o[0:64]
        for head in range(1, HEADS):
            mixed = jnp.where(masks[head], o[64 * head:64 * head + 64], mixed)
        mixes.append(mixed.astype(BF16))
    moved = nn(jnp.concatenate(mixes, axis=0), fw_ref[3]).astype(BF16).astype(F32)
    after = x_ref[...] + moved
    normed = norm(after).astype(BF16)

    def rows_of(v, f):
        return jnp.concatenate([v[64 * j + 16 * f:64 * j + 16 * f + 16] for j in range(RB // 16)], axis=0)

    for f in range(OWN):
        pack(zs, f, rows_of(normed, f))
        res[f * RB:(f + 1) * RB, :] = rows_of(after, f)
    z_copies = [remote(zs.at[lax.rem(z + d + NZ, OWN)], zr.at[slot], z_send.at[slot], z_recv.at[slot], dz(d))
                for slot, d in ((3, two), (1, 1), (2, -1))]
    for copy in z_copies:
        copy.start()
    zr[0] = zs[lax.rem(z, OWN)]
    for copy in z_copies:
        copy.wait_recv()

    n2 = jnp.concatenate([unpack(zr, k) for k in range(NS)], axis=0)
    keys = jnp.concatenate([n2[k * RB:k * RB + TR] for k in range(NS)], axis=0)
    kbuf[0, 0:KB, :] = keys[:, 0:128]
    kbuf[0, KB:BLOCK, :] = jnp.concatenate([keys[0:KB // 2, 128:E], keys[KB // 2:KB, 128:E]], axis=1)

    low, high = pl.ds(0, HALF), pl.ds(HALF, HALF)

    def send_block(slot, which, target, to_slot, rows, recv):
        src = kbuf.at[slot] if rows is None else kbuf.at[slot, rows]
        dst = kbuf.at[to_slot] if rows is None else kbuf.at[to_slot, rows]
        return remote(src, dst, own_send.at[slot, which], recv.at[to_slot], target)

    def sends(i):
        t, p, a = ORDER[i]
        out = []
        if (p, a) == (0, 0):
            out += [(2, y_pair, SLOT[t, 1, 0], None, ag_recv)]
        if a == 0:
            out += [(0, x_up, SLOT[t, p, 1], None, ag_recv), (1, x_down, SLOT[t, p, 2], None, ag_recv)]
        if a == 1:
            out += [(0, x_up, SLOT[t, p, 3], low, ag_recv)]
        if a == 2:
            out += [(1, x_down, SLOT[t, p, 3], high, ag_recv2)]
        return [send_block(i, *o) for o in out]

    def sib_copy(i):
        return remote(kbuf.at[i], kbuf.at[STEPS + i], sib_send.at[i], sib_recv.at[i], sibling)

    across = remote(kbuf.at[0], kbuf.at[SLOT[1, 0, 0]], far_send.at[0], ag_recv.at[SLOT[1, 0, 0]], dz(4))

    def handle(i):
        t, p, a = ORDER[i]
        if i:
            if a == 3:
                remote(kbuf.at[i, low], kbuf.at[i, low], own_send.at[i, 0], ag_recv.at[i], x_up).wait_recv()
                remote(kbuf.at[i, high], kbuf.at[i, high], own_send.at[i, 0], ag_recv2.at[i], x_up).wait_recv()
            else:
                remote(kbuf.at[i], kbuf.at[i], own_send.at[i, 0], ag_recv.at[i], x_up).wait_recv()
        for copy in sends(i):
            copy.start()
        sib_copy(i).start()

    across.start()
    handle(0)

    fetch[3].wait()
    fetch[4].wait()
    fetch[5].wait()
    q2 = nn(n2, rw_ref[0]).astype(BF16)
    wk = rw_ref[1]
    zero = jnp.zeros((E, E), BF16)
    for g in range(HEADS // 2):
        pair = [(nt(jnp.where(head_mask(E, 2 * g + k), wk, zero), q2) * SCALE).astype(BF16) for k in range(2)]
        pair = jnp.concatenate(pair, axis=1)
        for t in range(3):
            part = pair[:, UW * t:UW * t + UW]
            for k in range(2):
                qp[3 * g + t, k, 0:128, :] = part[0:128]
                qp[3 * g + t, k, 128 + 64 * k:192 + 64 * k, :] = part[128:E]
                qp[3 * g + t, k, 192 - 64 * k:256 - 64 * k, :] = jnp.zeros((64, UW), BF16)
    wvt = nt(eye(E), rw_ref[2]).astype(BF16)
    gap = jnp.zeros((E, 64), BF16)
    wv[0] = jnp.concatenate([wvt, gap], axis=1)
    wv[1] = jnp.concatenate([wvt[:, 0:128], gap, wvt[:, 128:E]], axis=1)
    va[...] = jnp.ones_like(va)
    acc[...] = jnp.zeros_like(acc)
    m_acc[...] = jnp.full_like(m_acc, FAR)
    m_new[...] = jnp.full_like(m_new, FAR)

    span = [(0, 48), (0, 80), (32, 80)]

    def blocks_of(i):
        if isinstance(i, int) and i == 0:
            return 0, STEPS
        one = jnp.where(i < STEPS - 1, i + 1, 2 * STEPS - 1)
        other = jnp.where(i == 1, 1, i + STEPS - 1)
        return (jnp.where(i == 3, STEPS + 3, jnp.where(i == 4, 4, one)), jnp.where(i == 4, 5, other))

    def half_keys(i, k):
        return jnp.concatenate([
            jnp.concatenate([kbuf[slot, 128 * k:128 * k + 128, :], kbuf[slot, KB:BLOCK, :]], axis=1)
            for slot in blocks_of(i)], axis=0)

    def score(i, u):
        for k in range(2):
            s = nn(half_keys(i, k), qp[u, k])
            sbuf[u, KB * k:KB * k + KB, :] = s
            m_new[u] = jnp.maximum(m_new[u], jnp.max(s, axis=0, keepdims=True))

    def weigh(u):
        lo, hi = span[u % 3]
        new = m_new[u]
        fade = jnp.exp2(m_acc[u] - new)
        m_acc[u] = new
        w = jnp.exp2(sbuf[u] - new).astype(BF16)
        acc[u, lo:hi, :] = acc[u, lo:hi, :] * fade + nn(va[u // 3, lo:hi, :], w)

    def values(i):
        for k in range(2):
            vt = nt(wv[k], half_keys(i, k)).astype(BF16)
            for g in range(3):
                va[g, 0:32, KB * k:KB * k + KB] = vt[64 * g:64 * g + 32]
                va[g, 48:80, KB * k:KB * k + KB] = vt[64 * g + 32:64 * g + 64]

    def arrive(i):
        remote(kbuf.at[0], kbuf.at[STEPS + i], sib_send.at[i], sib_recv.at[i], sibling).wait_recv()

    def advance(i, following):
        values(i)
        for u in range(UNITS):
            if u + 3 < UNITS:
                score(i, u + 3)
            elif following is not None:
                score(following, u + 3 - UNITS)
            weigh(u)

    arrive(0)
    score(0, 0)
    score(0, 1)
    score(0, 2)
    advance(0, None)
    handle(1)
    handle(2)
    score(1, 0)
    score(1, 1)
    score(1, 2)

    def step(i, carry):
        def pick(lo, hi):
            if hi - lo == 1:
                for k in {2: (), 3: (4, 5)}.get(lo, (lo + 2,)):
                    handle(k)
                return
            mid = (lo + hi) // 2
            pl.when(i < mid)(lambda: pick(lo, mid))
            pl.when(i >= mid)(lambda: pick(mid, hi))

        pl.when(i < STEPS - 2)(lambda: pick(1, STEPS - 2))

        @pl.when((i != 3) & (i < STEPS - 1))
        def _():
            arrive(i)

        @pl.when((i == 2) | (i == STEPS - 2))
        def _():
            arrive(i + 1)

        advance(i, jnp.minimum(i + 1, STEPS - 1))
        return carry

    lax.fori_loop(1, STEPS, step, 0)

    parts = []
    for g in range(3):
        o = [acc[3 * g + t] for t in range(3)]
        o = [v / v[32:33] for v in o]
        parts += [jnp.concatenate([o[0][0:32], o[1][0:32, 0:UW // 2]], axis=1),
                  jnp.concatenate([o[1][48:80, UW // 2:], o[2][48:80]], axis=1)]
    mix_t = jnp.concatenate(parts, axis=0).astype(BF16)
    mix = nt(eye(NQ), mix_t).astype(BF16)
    for k in range(NS):
        pack(os_ref, k, mix[k * RB:(k + 1) * RB])

    mine = lax.rem(z, OWN)
    o_copies = [remote(os_ref.at[slot], or_ref.at[mine], o_send.at[slot], o_recv.at[mine], dz(d))
                for slot, d in ((3, -two), (1, -1), (2, 1))]
    for copy in o_copies:
        copy.start()

    def finish(f, mixture):
        after_row = res[pl.ds(pl.multiple_of(f * RB, RB), RB), :] + nn(mixture, rw_ref[3])
        n3 = norm(after_row).astype(BF16)
        hidden = nn(n3, up_ref[...])
        hidden = (hidden * 0.5 * (1.0 + lax.erf(hidden * (2.0 ** -0.5)))).astype(BF16)
        fin[f] = (after_row + nt(hidden, down_ref[...])).astype(BF16)

    finish(mine, mix[0:RB])
    for d in (1, -1, 2):
        f = lax.rem(z + d + NZ, OWN)
        remote(os_ref.at[0], or_ref.at[f], o_send.at[0], o_recv.at[f], sibling).wait_recv()
        finish(f, unpack(or_ref, f))
    train_out[...] = jnp.concatenate([fin[f, 0:TR, :] for f in range(OWN)], axis=1)
    test_out[...] = jnp.concatenate([fin[f, TR:RB, :] for f in range(OWN)], axis=1)

    for copy in ex + z_copies + o_copies + [across]:
        copy.wait_send()
    for i in range(STEPS):
        for copy in sends(i):
            copy.wait_send()
        sib_copy(i).wait_send()


def body(*args):
    args = (*args[:5], args[5].T)
    train, test = args[0], args[1]
    dma = pltpu.SemaphoreType.DMA
    return pl.pallas_call(
        kernel,
        name="layer",
        out_shape=(pltpu.VMEM(train.shape, BF16), pltpu.VMEM(test.shape, BF16)),
        in_specs=[pl.BlockSpec(memory_space=pl.ANY)] * 6,
        out_specs=(pl.BlockSpec(memory_space=pltpu.VMEM),) * 2,
        scratch_shapes=[pltpu.VMEM(v.shape, BF16) for v in args] + [
            pltpu.VMEM((TR, OWN * E), BF16),
            pltpu.VMEM((TE, OWN * E), BF16),
            pltpu.VMEM((OWN * RB, E), F32),
            pltpu.VMEM((OWN * RB, E), F32),
            pltpu.VMEM((OWN, ZB, 128), BF16),
            pltpu.VMEM((NS, ZB, 128), BF16),
            pltpu.VMEM((2 * STEPS, BLOCK, 128), BF16),
            pltpu.VMEM((UNITS, 2, 256, UW), BF16),
            pltpu.VMEM((2, E, 256), BF16),
            pltpu.VMEM((3, 80, 2 * KB), BF16),
            pltpu.VMEM((UNITS, 2 * KB, UW), F32),
            pltpu.VMEM((UNITS, 80, UW), F32),
            pltpu.VMEM((UNITS, 1, UW), F32),
            pltpu.VMEM((UNITS, 1, UW), F32),
            pltpu.VMEM((NS, ZB, 128), BF16),
            pltpu.VMEM((OWN, ZB, 128), BF16),
            pltpu.VMEM((NQ, E), F32),
            pltpu.VMEM((OWN, RB, E), BF16),
            dma((2,)), dma((2,)), dma((NS,)), dma((NS,)),
            dma((STEPS, 4)), dma((STEPS,)), dma((STEPS,)), dma((STEPS,)), dma((STEPS,)),
            dma((NS,)), dma((OWN,)), dma((1,)), dma((6,)),
        ],
        compiler_params=pltpu.CompilerParams(
            collective_id=0, has_side_effects=True, vmem_limit_bytes=60 * 1024 * 1024),
    )(*args)


def solution(mesh):
    return jax.shard_map(
        body,
        mesh=mesh,
        in_specs=(P("rows", "feat"), P("rows", "feat"), P(), P(), P(), P()),
        out_specs=(P("rows", "feat"), P("rows", "feat")),
        check_vma=False,
    )
```
